32 devices in a mesh: rep: 8 (over y, x, core), tp: 4 (over z).
Axes of the slice: x: 2, y: 2, z: 4, core: 2. Of those that a mesh axis runs over, the one named last changes fastest.
Arguments:
- hidden: bfloat16 [512, 8192], P('rep'), may hold values from -6 to 6
- norm_gain: bfloat16 [8192], replicated, may hold values from 0.5 to 1.5
- query_weight_matrix: bfloat16 [8192, 4096], P(None, 'tp'), may hold values from -0.0625 to 0.0625
- key_value_weight: bfloat16 [2, 8192, 1024], P(None, None, 'tp'), may hold values from -0.0625 to 0.0625
- output_weight_matrix: bfloat16 [4096, 8192], P('tp'), may hold values from -0.375 to 0.375
- input_down_factors: bfloat16 [3, 8192, 64], P(None, ('rep', 'tp')), may hold values from -0.0625 to 0.0625
- query_up_factor: bfloat16 [64, 4096], P(None, ('rep', 'tp')), may hold values from -0.75 to 0.75
- key_value_up_factors: bfloat16 [2, 64, 1024], P(None, None, ('rep', 'tp')), may hold values from -0.75 to 0.75
- output_down_factor: bfloat16 [4096, 64], P(('rep', 'tp')), may hold values from -0.375 to 0.375
- output_up_factor: bfloat16 [64, 8192], P(None, ('rep', 'tp')), may hold values from -0.75 to 0.75
- cache_keys: bfloat16 [512, 8, 128, 128], P('rep', 'tp'), may hold values from -360 to 360
- cache_values: bfloat16 [512, 8, 128, 128], P('rep', 'tp'), may hold values from -6 to 6
- lengths: int32 [512], P('rep'), may hold values from 1 to 127
Outputs:
- attn_out: bfloat16 [512, 8192], P('rep', 'tp')
The draws below stay inside these ranges and needn't reach their ends.
All inputs are finite; a program needn't handle non-finite values.
Results may differ from the reference program's by a relative error of at most 0.03.
Values may be sent and summed in bfloat16 or wider, within the bound.
No kernel may reach another device: no remote copies, remote signals or barrier semaphores. Data moves between devices by JAX's collectives and lax.ppermute only.
A program may use at most 128 MiB of HBM per device.

```python
import math
import jax
import jax.numpy as jnp
from jax import lax

D = 8192
HEADS = 32
KV_HEADS = 8
HEAD_DIM = 128
RANK = 64
CACHE = 128
BATCH = 512


def draw_cache_keys(key, part):
    base_key = jax.random.fold_in(key, 11)
    values = jax.random.normal(base_key, (BATCH, KV_HEADS, CACHE, HEAD_DIM), jnp.float32)
    values = jnp.clip(values, -6.0, 6.0)
    return values.astype(jnp.bfloat16)


def set_ends(array, key, least, largest):
    spot = [jax.random.randint(jax.random.fold_in(key, axis), (), 0, length) for axis, length in enumerate(array.shape)]
    widest = array.shape.index(max(array.shape))
    next_to = spot[:widest] + [(spot[widest] + 1) % array.shape[widest]] + spot[widest + 1:]
    return array.at[tuple(spot)].set(least).at[tuple(next_to)].set(largest)


def levels(stream_key, dims, shards, least, largest):
    factor_of, own = 1.0, jax.random.fold_in(stream_key, 6)
    for axis_at, blocks in shards:
        heights = jnp.exp(jax.random.uniform(jax.random.fold_in(own, axis_at), (blocks,), jnp.float32, least / len(shards), largest / len(shards)))
        factor_of = factor_of * jnp.repeat(heights, dims[axis_at] // blocks).reshape([-1 if axis == axis_at else 1 for axis in range(len(dims))])
    return factor_of


def normal_values(rng, extent, scale, most, pieces=(), held_as=jnp.bfloat16):
    entries = jax.random.normal(rng, extent, jnp.float32) * scale
    if len(pieces) > 0:
        entries = levels(rng, extent, pieces, -0.22, 0.18) * entries
    return jnp.clip(entries, min=-most, max=most).astype(held_as)


def setup_inputs(seed: int = 0) -> dict:
    key_list = jax.random.split(jax.random.key(seed), 14)
    hidden = normal_values(key_list[0], (BATCH, D), 1.0, 6.0, ((0, 8),))
    norm_gain = jnp.clip(1.0 + 0.1 * jax.random.normal(key_list[1], (D,), jnp.float32), 0.5, 1.5).astype(jnp.bfloat16)
    query_weight_matrix = normal_values(key_list[2], (D, HEADS * HEAD_DIM), D ** -0.5, 0.0625, ((1, 4),))
    key_value_weight = normal_values(key_list[3], (2, D, KV_HEADS * HEAD_DIM), D ** -0.5, 0.0625, ((2, 4),))
    output_weight_matrix = normal_values(key_list[4], (HEADS * HEAD_DIM, D), (HEADS * HEAD_DIM // 16) ** -0.5, 0.375, ((0, 4),))
    input_down_factors = normal_values(key_list[5], (3, D, RANK), D ** -0.5, 0.0625, ((1, 32),))
    query_up_factor = normal_values(key_list[6], (RANK, HEADS * HEAD_DIM), RANK ** -0.5, 0.75, ((1, 32),))
    key_value_up_factors = normal_values(key_list[7], (2, RANK, KV_HEADS * HEAD_DIM), RANK ** -0.5, 0.75, ((2, 32),))
    output_down_factor = normal_values(key_list[8], (HEADS * HEAD_DIM, RANK), (HEADS * HEAD_DIM // 16) ** -0.5, 0.375, ((0, 32),))
    output_up_factor = normal_values(key_list[9], (RANK, D), RANK ** -0.5, 0.75, ((1, 32),))
    cache_keys = draw_cache_keys(jax.random.fold_in(key_list[13], 71), 0)
    cache_values = normal_values(key_list[11], (BATCH, KV_HEADS, CACHE, HEAD_DIM), 1.0, 6.0, ((0, 8), (1, 4)))
    lengths = set_ends(jax.random.randint(key_list[12], (BATCH,), 1, CACHE), jax.random.fold_in(key_list[12], 1), 1, CACHE - 1).astype(jnp.int32)
    return dict(hidden=hidden, norm_gain=norm_gain, query_weight_matrix=query_weight_matrix, key_value_weight=key_value_weight, output_weight_matrix=output_weight_matrix, input_down_factors=input_down_factors, query_up_factor=query_up_factor, key_value_up_factors=key_value_up_factors, output_down_factor=output_down_factor, output_up_factor=output_up_factor, cache_keys=cache_keys, cache_values=cache_values, lengths=lengths)


epsilon = 1e-06
rope_base = 1000000.0
adapter_scale = 0.5

def rope_angles(lengths, head_dim):
    half_dim = head_dim // 2
    frequency = rope_base ** (-(jnp.arange(half_dim, dtype=jnp.float32) * 2.0) / head_dim)
    return lengths.astype(jnp.float32)[:, None] * frequency[None, :]

def rotate(vectors, angles):
    half_dim = vectors.shape[-1] // 2
    cosine = jnp.cos(angles)[:, None, :]
    sine_part = jnp.sin(angles)[:, None, :]
    low_half = vectors[..., :half_dim]
    high_half = vectors[..., half_dim:]
    return jnp.concatenate([low_half * cosine - high_half * sine_part, high_half * cosine + low_half * sine_part], axis=-1)

def adapted(normed, frozen_matrix, inner_part, up_factor):
    base_part = jnp.dot(normed, frozen_matrix, preferred_element_type=jnp.float32)
    return base_part + adapter_scale * jnp.dot(inner_part, up_factor, preferred_element_type=jnp.float32)

def attend(query, new_key, new_value, keys, values, lengths):
    score_scale = 1.0 / math.sqrt(keys.shape[-1])
    scores = jnp.einsum('bkgd,bkld->bkgl', query, keys.astype(jnp.float32), precision=lax.Precision.HIGHEST) * score_scale
    own_score = lax.optimization_barrier(jnp.sum(query * new_key.astype(jnp.float32)[:, :, None, :], axis=-1)) * score_scale
    live_mask = jnp.arange(keys.shape[2], dtype=jnp.int32)[None, None, None, :] < lengths[:, None, None, None]
    row_max = jnp.maximum(lax.optimization_barrier(jnp.max(jnp.where(live_mask, scores, -1e+30), axis=-1)), own_score)
    weights = jnp.where(live_mask, jnp.exp(scores - row_max[..., None]), 0.0)
    own_weight = jnp.exp(own_score - row_max)
    denom_sum = lax.optimization_barrier(jnp.sum(weights, axis=-1)) + own_weight
    probs = (weights / denom_sum[..., None]).astype(jnp.bfloat16)
    own_prob = (own_weight / denom_sum).astype(jnp.bfloat16)
    context = jnp.einsum('bkgl,bkld->bkgd', probs.astype(jnp.float32), values.astype(jnp.float32))
    context = context + own_prob.astype(jnp.float32)[..., None] * new_value.astype(jnp.float32)[:, :, None, :]
    return context.astype(jnp.bfloat16)

def reference(hidden, norm_gain, query_weight_matrix, key_value_weight, output_weight_matrix, input_down_factors, query_up_factor, key_value_up_factors, output_down_factor, output_up_factor, cache_keys, cache_values, lengths):
    states = hidden.astype(jnp.float32)
    square = lax.optimization_barrier(jnp.mean(states * states, axis=-1, keepdims=True))
    normed = (states * lax.rsqrt(square + epsilon) * norm_gain.astype(jnp.float32)).astype(jnp.bfloat16)
    inner_query = jnp.dot(normed, input_down_factors[0], preferred_element_type=jnp.float32).astype(jnp.bfloat16)
    inner_key = jnp.dot(normed, input_down_factors[1], preferred_element_type=jnp.float32).astype(jnp.bfloat16)
    inner_value = jnp.dot(normed, input_down_factors[2], preferred_element_type=jnp.float32).astype(jnp.bfloat16)
    batch = hidden.shape[0]
    kv_count = cache_keys.shape[1]
    head_dim = cache_keys.shape[3]
    angles = rope_angles(lengths, head_dim)
    query = adapted(normed, query_weight_matrix, inner_query, query_up_factor).reshape(batch, -1, head_dim)
    query = rotate(query, angles).reshape(batch, kv_count, -1, head_dim)
    new_key = adapted(normed, key_value_weight[0], inner_key, key_value_up_factors[0]).reshape(batch, kv_count, head_dim)
    new_key = rotate(new_key, angles).astype(jnp.bfloat16)
    new_value = adapted(normed, key_value_weight[1], inner_value, key_value_up_factors[1]).reshape(batch, kv_count, head_dim).astype(jnp.bfloat16)
    context = attend(query, new_key, new_value, cache_keys, cache_values, lengths).reshape(batch, -1)
    middle = jnp.dot(context, output_down_factor, preferred_element_type=jnp.float32).astype(jnp.bfloat16)
    return adapted(context, output_weight_matrix, middle, output_up_factor).astype(jnp.bfloat16)
```

```python
import functools
import math

import jax
import jax.numpy as jnp
from jax import lax
from jax.experimental import pallas as pl
from jax.experimental.pallas import tpu as pltpu
from jax.sharding import PartitionSpec as P

epsilon = 1e-06
rope_base = 1000000.0
adapter_scale = 0.5
F32 = jnp.float32
BF16 = jnp.bfloat16


def params(mib=24):
    return pltpu.CompilerParams(vmem_limit_bytes=mib * 1024 * 1024)


def whole(shape):
    return pl.BlockSpec(shape, lambda *_: (0,) * len(shape))


def tables(lengths, head_dim):
    half_dim = head_dim // 2
    frequency = rope_base ** (-(jnp.arange(half_dim, dtype=F32) * 2.0) / head_dim)
    angles = lengths.astype(F32)[:, None] * frequency[None, :]
    cosine, sine = jnp.cos(angles), jnp.sin(angles)
    return jnp.concatenate([cosine, cosine], 1), jnp.concatenate([-sine, sine], 1)


def power_of_two(n):
    return n & (n - 1) == 0


def exchange(n):
    if power_of_two(n):
        return lambda i, k: i ^ k
    return lambda i, k: (i + k) % n


def hop(x, axis, k):
    n = lax.axis_size(axis)
    to = exchange(n)
    return lax.ppermute(x, axis, [(i, to(i, k)) for i in range(n)])


def came_from(index, n, k):
    if power_of_two(n):
        return index ^ k
    return (index - k) % n


def gather_rep(block):
    n = lax.axis_size("rep")
    r = lax.axis_index("rep")
    if not power_of_two(n) or n == 1:
        return [block] + [hop(block, "rep", k) for k in range(1, n)], [
            came_from(r, n, k) for k in range(n)
        ]
    near = [block] + [hop(block, "rep", k) for k in range(2, n, 2)]
    order = [r ^ k for k in range(0, n, 2)]
    return near + [hop(b, "rep", 1) for b in near], order + [o ^ 1 for o in order]


def norm_kernel(hidden_ref, gain_ref, out_ref):
    states = hidden_ref[...].astype(F32)
    square = jnp.mean(states * states, axis=-1, keepdims=True)
    scaled = states * lax.rsqrt(square + epsilon) * gain_ref[...].astype(F32)
    out_ref[...] = scaled.astype(BF16)


def normalize(hidden, gain):
    rows, wide = hidden.shape
    step = 16 if rows % 16 == 0 else rows
    return pl.pallas_call(
        norm_kernel,
        grid=(rows // step,),
        in_specs=[pl.BlockSpec((step, wide), lambda i: (i, 0)), whole((1, wide))],
        out_specs=pl.BlockSpec((step, wide), lambda i: (i, 0)),
        out_shape=jax.ShapeDtypeStruct((rows, wide), BF16),
        compiler_params=params(8),
        name="norm",
    )(hidden, gain[None])


def base_kernel(x_ref, q_ref, kv_ref, q_out, k_out, v_out):
    @pl.when(pl.program_id(0) == 0)
    def _():
        q_out[...] = jnp.zeros_like(q_out)
        k_out[...] = jnp.zeros_like(k_out)
        v_out[...] = jnp.zeros_like(v_out)

    x = x_ref[...]
    q_out[...] += jnp.dot(x, q_ref[...], preferred_element_type=F32)
    k_out[...] += jnp.dot(x, kv_ref[0], preferred_element_type=F32)
    v_out[...] += jnp.dot(x, kv_ref[1], preferred_element_type=F32)


def base_projections(normed, query_weights, key_value_weights):
    rows, wide = normed.shape
    q_cols = query_weights.shape[1]
    kv_cols = key_value_weights.shape[2]
    step = 512
    return pl.pallas_call(
        base_kernel,
        grid=(wide // step,),
        in_specs=[
            pl.BlockSpec((rows, step), lambda i: (0, i)),
            pl.BlockSpec((step, q_cols), lambda i: (i, 0)),
            pl.BlockSpec((2, step, kv_cols), lambda i: (0, i, 0)),
        ],
        out_specs=[whole((rows, q_cols)), whole((rows, kv_cols)), whole((rows, kv_cols))],
        out_shape=[
            jax.ShapeDtypeStruct((rows, q_cols), F32),
            jax.ShapeDtypeStruct((rows, kv_cols), F32),
            jax.ShapeDtypeStruct((rows, kv_cols), F32),
        ],
        compiler_params=params(16),
        cost_estimate=pl.CostEstimate(
            flops=2 * rows * wide * (q_cols + 2 * kv_cols),
            bytes_accessed=2 * wide * (q_cols + 2 * kv_cols),
            transcendentals=0,
        ),
        name="base",
    )(normed, query_weights, key_value_weights)


def pack_down(down):
    half = down.shape[1] // 2
    return jnp.concatenate(
        [p for j in range(down.shape[0]) for p in (down[j, :half], down[j, half:])], axis=1
    )


def inner_kernel(starts_ref, x_ref, *refs):
    blocks, out_ref = refs[:-1], refs[-1]
    half, wide = blocks[0].shape
    rank = wide // 6
    first = jnp.zeros((x_ref.shape[0], wide), F32)
    second = jnp.zeros((x_ref.shape[0], wide), F32)
    for j, block in enumerate(blocks):
        at = pl.multiple_of(starts_ref[j] * (2 * half), 2 * half)
        first += jnp.dot(x_ref[:, pl.ds(at, half)], block[...], preferred_element_type=F32)
        second += jnp.dot(
            x_ref[:, pl.ds(at + half, half)], block[...], preferred_element_type=F32
        )
    sums = [
        first[:, 2 * j * rank : (2 * j + 1) * rank]
        + second[:, (2 * j + 1) * rank : (2 * j + 2) * rank]
        for j in range(3)
    ]
    sums.append(jnp.zeros_like(sums[0]))
    out_ref[...] = jnp.concatenate(sums, axis=1).astype(BF16)


def partial_inner(normed, blocks, places):
    half, wide = blocks[0].shape
    rank = wide // 6
    rows = normed.shape[0]
    if half % 128 == 0 and wide % 128 == 0:
        return pl.pallas_call(
            inner_kernel,
            grid_spec=pltpu.PrefetchScalarGridSpec(
                num_scalar_prefetch=1,
                grid=(1,),
                in_specs=[whole(normed.shape)] + [whole(b.shape) for b in blocks],
                out_specs=whole((rows, 4 * rank)),
            ),
            out_shape=jax.ShapeDtypeStruct((rows, 4 * rank), BF16),
            compiler_params=params(8),
            cost_estimate=pl.CostEstimate(
                flops=4 * rows * half * wide * len(blocks),
                bytes_accessed=2 * half * wide * len(blocks),
                transcendentals=0,
            ),
            name="inner",
        )(jnp.stack(places).astype(jnp.int32), normed, *blocks)
    sums = [jnp.zeros((rows, rank), F32) for _ in range(3)]
    for place, block in zip(places, blocks):
        own = lax.dynamic_slice_in_dim(normed, place * 2 * half, 2 * half, 1)
        for j in range(3):
            for part in range(2):
                lane = (2 * j + part) * rank
                sums[j] += jnp.dot(
                    own[:, part * half : (part + 1) * half],
                    block[:, lane : lane + rank],
                    preferred_element_type=F32,
                )
    sums.append(jnp.zeros_like(sums[0]))
    return jnp.concatenate(sums, 1).astype(BF16)


def assemble_kernel(order_ref, *refs, widths, count):
    blocks, outs = refs[:count], refs[count:]
    offset = 0
    for width, out_ref in zip(widths, outs):
        total = out_ref.shape[1]
        if width % 128 == 0:
            for j, block in enumerate(blocks):
                at = pl.multiple_of(order_ref[j] * width, 128)
                out_ref[:, pl.ds(at, width)] = block[:, offset : offset + width]
        else:
            placed = jnp.zeros((out_ref.shape[0], total), F32)
            source = lax.broadcasted_iota(jnp.int32, (width, total), 0)
            target = lax.broadcasted_iota(jnp.int32, (width, total), 1)
            for j, block in enumerate(blocks):
                chosen = (target == source + order_ref[j] * width).astype(BF16)
                placed += jnp.dot(
                    block[:, offset : offset + width], chosen, preferred_element_type=F32
                )
            out_ref[...] = placed.astype(BF16)
        offset += width


def assemble(blocks, order, widths):
    rank = blocks[0].shape[0]
    count = len(blocks)
    return pl.pallas_call(
        functools.partial(assemble_kernel, widths=widths, count=count),
        grid_spec=pltpu.PrefetchScalarGridSpec(
            num_scalar_prefetch=1,
            grid=(1,),
            in_specs=[whole(b.shape) for b in blocks],
            out_specs=[whole((rank, w * count)) for w in widths],
        ),
        out_shape=[jax.ShapeDtypeStruct((rank, w * count), BF16) for w in widths],
        compiler_params=params(8),
        name="assemble",
    )(jnp.stack(order).astype(jnp.int32), *blocks)


def attend_kernel(
    lengths_ref, q_ref, k_ref, v_ref, parts_ref, q_up, k_up, v_up, od_ref, cos_ref, sin_ref,
    *refs, parts, group,
):
    others = refs[: parts - 1]
    keys_ref, values_ref, ctx_ref, pm_ref, q3, own, nv, cs = refs[parts - 1 :]
    rows, dim = cos_ref.shape
    heads = q_ref.shape[1] // dim
    kv = heads // group
    rank = q_up.shape[0]
    block = keys_ref.shape[0]
    scale = 1.0 / math.sqrt(dim)
    step = pl.program_id(0)

    @pl.when(step == 0)
    def _():
        total = parts_ref[...].astype(F32)
        for other in others:
            total += other[...].astype(F32)
        inner = total.astype(BF16)
        cosine, sine = cos_ref[...], sin_ref[...]

        def turned(x):
            return x * cosine + pltpu.roll(x, dim // 2, 1) * sine

        def added(base_ref, j, up, h):
            lane = slice(h * dim, (h + 1) * dim)
            return base_ref[:, lane] + adapter_scale * jnp.dot(
                inner[:, j * rank : (j + 1) * rank], up[:, lane], preferred_element_type=F32
            )

        for g in range(kv):
            key = turned(added(k_ref, 1, k_up, g)).astype(BF16).astype(F32)
            value = added(v_ref, 2, v_up, g).astype(BF16).astype(F32)
            for h in range(g * group, (g + 1) * group):
                x = turned(added(q_ref, 0, q_up, h))
                score = jnp.sum(x * key, axis=-1, keepdims=True) * scale
                own[:, h, :] = jnp.broadcast_to(score, (rows, dim))
                nv[:, h, :] = value
                high = x.astype(BF16).astype(F32)
                rest = x - high
                mid = rest.astype(BF16).astype(F32)
                q3[:, h, :] = high
                q3[:, heads + h, :] = mid
                q3[:, 2 * heads + h, :] = rest - mid

    row = lax.broadcasted_iota(jnp.int32, (heads, dim), 0)
    positions = keys_ref.shape[2]
    spot = lax.broadcasted_iota(jnp.int32, (heads, positions), 1)

    def select(pieces):
        out = pieces[0]
        for g in range(1, kv):
            out = jnp.where(row >= g * group, pieces[g], out)
        return out

    for b in range(block):
        s = step * block + b
        q = q3[s].astype(BF16)
        pieces = []
        for g in range(kv):
            full = lax.dot_general(
                q, keys_ref[b, g], (((1,), (1,)), ((), ())), preferred_element_type=F32
            )
            pieces.append(
                full[:heads] + (full[heads : 2 * heads] + full[2 * heads :])
            )
        live = spot < lengths_ref[s]
        scores = select(pieces) * scale
        own_score = own[s]
        top = jnp.maximum(
            jnp.max(jnp.where(live, scores, -1e30), axis=-1, keepdims=True), own_score
        )
        weights = jnp.where(live, jnp.exp(scores - top), 0.0)
        own_weight = jnp.exp(own_score - top)
        denom = jnp.sum(weights, axis=-1, keepdims=True) + own_weight
        probs = (weights / denom).astype(BF16)
        own_prob = (own_weight / denom).astype(BF16).astype(F32)
        pieces = [
            jnp.dot(probs, values_ref[b, g], preferred_element_type=F32) for g in range(kv)
        ]
        cs[s] = select(pieces) + own_prob * nv[s]

    @pl.when(step == pl.num_programs(0) - 1)
    def _():
        middle = jnp.zeros((rows, rank), F32)
        for h in range(heads):
            lane = slice(h * dim, (h + 1) * dim)
            context = cs[:, h, :].astype(BF16)
            ctx_ref[:, lane] = context
            middle += lax.dot_general(
                context, od_ref[:, lane], (((1,), (1,)), ((), ())), preferred_element_type=F32
            )
        high = middle.astype(BF16)
        low = (middle - high.astype(F32)).astype(BF16)
        pm_ref[...] = jnp.concatenate([high, low], axis=1)


def attention(lengths, base, parts, ups, od, angles, keys, values):
    rows, kv, positions, dim = keys.shape
    q_cols = base[0].shape[1]
    heads = q_cols // dim
    rank = od.shape[0]
    block = 8 if rows % 8 == 0 else rows
    cache_spec = pl.BlockSpec((block, kv, positions, dim), lambda i, *_: (i, 0, 0, 0))
    fixed = list(base) + [parts[0]] + list(ups) + [od] + list(angles) + list(parts[1:])
    return pl.pallas_call(
        functools.partial(attend_kernel, parts=len(parts), group=heads // kv),
        grid_spec=pltpu.PrefetchScalarGridSpec(
            num_scalar_prefetch=1,
            grid=(rows // block,),
            in_specs=[whole(a.shape) for a in fixed] + [cache_spec, cache_spec],
            out_specs=[whole((rows, q_cols)), whole((rows, 2 * rank))],
            scratch_shapes=[
                pltpu.VMEM((rows, 3 * heads, dim), F32),
                pltpu.VMEM((rows, heads, dim), F32),
                pltpu.VMEM((rows, heads, dim), F32),
                pltpu.VMEM((rows, heads, dim), F32),
            ],
        ),
        out_shape=[
            jax.ShapeDtypeStruct((rows, q_cols), BF16),
            jax.ShapeDtypeStruct((rows, 2 * rank), BF16),
        ],
        compiler_params=params(16),
        cost_estimate=pl.CostEstimate(
            flops=4 * rows * heads * positions * dim * 16,
            bytes_accessed=4 * keys.size,
            transcendentals=rows * heads * positions,
        ),
        name="attend",
    )(lengths, *fixed, keys, values)


def chunk_kernel(_, ctx_ref, w_ref, pm_ref, out_ref, *, step):
    i = pl.program_id(0)
    lane = pl.multiple_of(i * step, step)
    part = jnp.dot(ctx_ref[...], w_ref[...], preferred_element_type=F32)
    out_ref[:, pl.ds(lane, step)] = part.astype(out_ref.dtype)

    @pl.when(i == pl.num_programs(0) - 1)
    def _():
        wide = step * pl.num_programs(0)
        if out_ref.dtype == BF16:
            out_ref[:, -pm_ref.shape[1] :] = pm_ref[...]


def chunk(context, weights, middle, target, tp, dtype):
    rows, depth = context.shape
    wide = weights.shape[1] // tp
    step = 512 if wide % 512 == 0 else wide
    per = wide // step
    tail = middle.shape[1] if dtype == BF16 else 0
    return pl.pallas_call(
        functools.partial(chunk_kernel, step=step),
        grid_spec=pltpu.PrefetchScalarGridSpec(
            num_scalar_prefetch=1,
            grid=(per,),
            in_specs=[
                whole(context.shape),
                pl.BlockSpec((depth, step), lambda i, at: (0, at[0] * per + i)),
                whole(middle.shape),
            ],
            out_specs=whole((rows, wide + tail)),
        ),
        out_shape=jax.ShapeDtypeStruct((rows, wide + tail), dtype),
        compiler_params=params(8),
        cost_estimate=pl.CostEstimate(
            flops=2 * rows * depth * wide, bytes_accessed=2 * depth * wide, transcendentals=0
        ),
        name="chunk",
    )(target[None].astype(jnp.int32), context, weights, middle)


def final_kernel(own_ref, pm_ref, up_ref, *refs):
    others, out_ref = refs[:-1], refs[-1]
    wide = own_ref.shape[1]
    rank = up_ref.shape[0]
    total = own_ref[...]
    middle = pm_ref[:, :rank].astype(F32) + pm_ref[:, rank:].astype(F32)
    for other in others:
        total += other[:, :wide].astype(F32)
        tail = other[:, wide:].astype(F32)
        middle += tail[:, :rank] + tail[:, rank:]
    total += adapter_scale * jnp.dot(
        middle.astype(BF16), up_ref[...], preferred_element_type=F32
    )
    out_ref[...] = total.astype(BF16)


def finish(own, middle, out_up, others):
    args = [own, middle, out_up] + others
    return pl.pallas_call(
        final_kernel,
        grid=(1,),
        in_specs=[whole(a.shape) for a in args],
        out_specs=whole(own.shape),
        out_shape=jax.ShapeDtypeStruct(own.shape, BF16),
        compiler_params=params(8),
        name="final",
    )(*args)


def local(
    hidden,
    norm_gain,
    query_weight_matrix,
    key_value_weight,
    output_weight_matrix,
    input_down_factors,
    query_up_factor,
    key_value_up_factors,
    output_down_factor,
    output_up_factor,
    cache_keys,
    cache_values,
    lengths,
):
    rep = lax.axis_size("rep")
    tp = lax.axis_size("tp")
    t = lax.axis_index("tp")

    down_blocks, down_order = gather_rep(pack_down(input_down_factors))

    pieces = [
        query_up_factor,
        output_down_factor.T,
        output_up_factor,
        key_value_up_factors[0],
        key_value_up_factors[1],
    ]
    widths = tuple(p.shape[1] for p in pieces)
    packed = jnp.concatenate(pieces, axis=1)
    moved = lax.ppermute(
        packed, ("rep", "tp"), [(b, (b % rep) * tp + b // rep) for b in range(rep * tp)]
    )
    up_blocks, up_order = gather_rep(moved)

    angles = tables(lengths, cache_keys.shape[3])
    normed = normalize(hidden, norm_gain)
    base = base_projections(normed, query_weight_matrix, key_value_weight)
    part = partial_inner(normed, down_blocks, [o * tp + t for o in down_order])
    parts = [part] + [hop(part, "tp", k) for k in range(1, tp)]
    q_up, od, out_up, k_up, v_up = assemble(up_blocks, up_order, widths)
    context, middle = attention(
        lengths, base, parts, (q_up, k_up, v_up), od, angles, cache_keys, cache_values
    )
    to = exchange(tp)
    others = []
    for k in range(tp - 1, 0, -1):
        piece = chunk(context, output_weight_matrix, middle, to(t, k), tp, BF16)
        others.append(hop(piece, "tp", k))
    own = chunk(context, output_weight_matrix, middle, t, tp, F32)
    return finish(own, middle, out_up, others)


def solution(mesh):
    return jax.shard_map(
        local,
        mesh=mesh,
        in_specs=(
            P("rep", None),
            P(),
            P(None, "tp"),
            P(None, None, "tp"),
            P("tp", None),
            P(None, ("rep", "tp"), None),
            P(None, ("rep", "tp")),
            P(None, None, ("rep", "tp")),
            P(("rep", "tp"), None),
            P(None, ("rep", "tp")),
            P("rep", "tp", None, None),
            P("rep", "tp", None, None),
            P("rep"),
        ),
        out_specs=P("rep", "tp"),
        check_vma=False,
    )
```

```python
import functools
import math

import jax
import jax.numpy as jnp
from jax import lax
from jax.experimental import pallas as pl
from jax.experimental.pallas import tpu as pltpu
from jax.sharding import PartitionSpec as P


epsilon = 1e-06
rope_base = 1000000.0
adapter_scale = 0.5
F32 = jnp.float32
BF16 = jnp.bfloat16


def params(mib=24):
    return pltpu.CompilerParams(vmem_limit_bytes=mib * 1024 * 1024)


def whole(shape):
    return pl.BlockSpec(shape, lambda *_: (0,) * len(shape))


def power_of_two(n):
    return n & (n - 1) == 0


def exchange(n):
    if power_of_two(n):
        return lambda i, k: i ^ k
    return lambda i, k: (i + k) % n


def hop(x, axis, k):
    n = lax.axis_size(axis)
    to = exchange(n)
    return lax.ppermute(x, axis, [(i, to(i, k)) for i in range(n)])


def came_from(index, n, k):
    if power_of_two(n):
        return index ^ k
    return (index - k) % n


def gather_rep(block):
    n = lax.axis_size("rep")
    r = lax.axis_index("rep")
    if not power_of_two(n) or n == 1:
        return [block] + [hop(block, "rep", k) for k in range(1, n)], [
            came_from(r, n, k) for k in range(n)
        ]
    near = [block] + [hop(block, "rep", k) for k in range(2, n, 2)]
    order = [r ^ k for k in range(0, n, 2)]
    return near + [hop(b, "rep", 1) for b in near], order + [o ^ 1 for o in order]


def pack_kernel(q_ref, od_ref, ou_ref, kv_ref, out_ref):
    both = jnp.concatenate([kv_ref[0], kv_ref[1]], axis=0).astype(F32).T.astype(BF16)
    lane = 0
    for piece in (q_ref[...], od_ref[...], ou_ref[...], both):
        out_ref[:, lane : lane + piece.shape[1]] = piece
        lane += piece.shape[1]


def pack(q_up, od, ou, kv_up):
    widths = (q_up.shape[1], od.shape[0], ou.shape[1], kv_up.shape[2], kv_up.shape[2])
    if any(w % 128 for w in widths[:3]):
        return jnp.concatenate([q_up, od.T, ou, kv_up[0], kv_up[1]], axis=1), widths
    vmem = pl.BlockSpec(memory_space=pltpu.VMEM)
    packed = pl.pallas_call(
        pack_kernel,
        in_specs=[vmem] * 4,
        out_specs=vmem,
        out_shape=jax.ShapeDtypeStruct((q_up.shape[0], sum(widths)), BF16),
        compiler_params=params(60),
        name="pack",
    )(q_up, od.T, ou, kv_up.transpose(0, 2, 1))
    return packed, widths


def base_kernel(
    lengths_ref, gain_ref, hidden_hbm, q_hbm, kv_hbm, x_ref, cos_ref, sin_ref, q_out, kv_out,
    hidden, q_held, kv_held, angle, first_sem, q_sems, kv_sems,
):
    count, depth = q_held.shape[0], q_held.shape[1]
    rows, wide = hidden.shape

    def q_copy(i):
        return pltpu.make_async_copy(
            q_hbm.at[pl.ds(i * depth, depth), :], q_held.at[i], q_sems.at[i]
        )

    def kv_copy(i):
        return pltpu.make_async_copy(
            kv_hbm.at[:, pl.ds(i * depth, depth), :], kv_held.at[i], kv_sems.at[i]
        )

    first = pltpu.make_async_copy(hidden_hbm, hidden, first_sem)
    lead = min(4, count)
    first.start()
    for i in range(lead):
        q_copy(i).start()
        kv_copy(i).start()

    dim = cos_ref.shape[1]
    spot = lax.broadcasted_iota(jnp.int32, (1, dim), 1) % (dim // 2)
    freq = jnp.ones((1, dim), F32)
    for bit in range((dim // 2 - 1).bit_length()):
        power = rope_base ** (-(2.0 ** (bit + 1)) / dim)
        freq *= jnp.where((spot >> bit) % 2 == 1, power, 1.0)
    for s in range(rows):
        angle[s : s + 1, :] = freq * lengths_ref[s].astype(F32)
    low = lax.broadcasted_iota(jnp.int32, (rows, dim), 1) < dim // 2
    wave = jnp.sin(angle[...] + jnp.where(low, 0.0, math.pi / 2))
    other = pltpu.roll(wave, dim // 2, 1)
    cos_ref[...] = jnp.where(low, other, wave)
    sin_ref[...] = jnp.where(low, -wave, other)
    q_out[...] = jnp.zeros_like(q_out)
    kv_out[...] = jnp.zeros_like(kv_out)

    first.wait()
    part = gain_ref.shape[1]
    square = jnp.zeros((rows, part), F32)
    for j in range(wide // part):
        states = hidden[:, j * part : (j + 1) * part].astype(F32)
        square += states * states
    factor = lax.rsqrt(jnp.sum(square, axis=-1, keepdims=True) / wide + epsilon)
    for j in range(wide // part):
        lane = slice(j * part, (j + 1) * part)
        scaled = hidden[:, lane].astype(F32) * factor * gain_ref[j : j + 1, :].astype(F32)
        x_ref[:, lane] = scaled.astype(BF16)

    def step(i):
        x = x_ref[:, pl.ds(pl.multiple_of(i * depth, depth), depth)]
        q_copy(i).wait()
        q_out[...] += jnp.dot(x, q_held[i], preferred_element_type=F32)
        kv_copy(i).wait()
        for j in range(kv_hbm.shape[0]):
            kv_out[j] += jnp.dot(x, kv_held[i, j], preferred_element_type=F32)
        return 0

    def fed(i, _):
        @pl.when(i + lead < count)
        def _():
            q_copy(i + lead).start()
            kv_copy(i + lead).start()

        return step(i)

    lax.fori_loop(0, count, fed, 0)


def base_projections(hidden, gain, lengths, q_weights, kv_weights, dim):
    rows, wide = hidden.shape
    depth = 512
    count = wide // depth
    q_cols, kv_cols = q_weights.shape[1], kv_weights.shape[2]
    pair = kv_weights.shape[0]
    vmem = pl.BlockSpec(memory_space=pltpu.VMEM)
    hbm = pl.BlockSpec(memory_space=pltpu.HBM)
    return pl.pallas_call(
        base_kernel,
        in_specs=[pl.BlockSpec(memory_space=pltpu.SMEM), vmem, hbm, hbm, hbm],
        out_specs=[vmem] * 5,
        out_shape=[
            jax.ShapeDtypeStruct((rows, wide), BF16),
            jax.ShapeDtypeStruct((rows, dim), F32),
            jax.ShapeDtypeStruct((rows, dim), F32),
            jax.ShapeDtypeStruct((rows, q_cols), F32),
            jax.ShapeDtypeStruct((pair, rows, kv_cols), F32),
        ],
        scratch_shapes=[
            pltpu.VMEM((rows, wide), BF16),
            pltpu.VMEM((count, depth, q_cols), BF16),
            pltpu.VMEM((count, pair, depth, kv_cols), BF16),
            pltpu.VMEM((rows, dim), F32),
            pltpu.SemaphoreType.DMA(()),
            pltpu.SemaphoreType.DMA((count,)),
            pltpu.SemaphoreType.DMA((count,)),
        ],
        compiler_params=params(52),
        cost_estimate=pl.CostEstimate(
            flops=16 * rows * (q_weights.size + kv_weights.size),
            bytes_accessed=2 * (q_weights.size + kv_weights.size),
            transcendentals=0,
        ),
        name="base",
    )(lengths, gain.reshape(wide // 128, 128), hidden, q_weights, kv_weights)


def inner_kernel(starts_ref, x_ref, *refs):
    blocks, out_ref = refs[:-1], refs[-1]
    ranks, deep = blocks[0].shape
    total = jnp.zeros((x_ref.shape[0], ranks), F32)
    for j, block in enumerate(blocks):
        at = pl.multiple_of(starts_ref[j] * deep, deep)
        total += lax.dot_general(
            x_ref[:, pl.ds(at, deep)],
            block[...],
            (((1,), (1,)), ((), ())),
            preferred_element_type=F32,
        )
    rest = jnp.zeros((x_ref.shape[0], out_ref.shape[1] - ranks), F32)
    out_ref[...] = jnp.concatenate([total, rest], axis=1).astype(BF16)


def partial_inner(normed, blocks, places):
    ranks, deep = blocks[0].shape
    rows = normed.shape[0]
    padded = -(-ranks // 128) * 128
    if deep % 128 == 0:
        return pl.pallas_call(
            inner_kernel,
            grid_spec=pltpu.PrefetchScalarGridSpec(
                num_scalar_prefetch=1,
                grid=(1,),
                in_specs=[whole(normed.shape)] + [whole(b.shape) for b in blocks],
                out_specs=whole((rows, padded)),
            ),
            out_shape=jax.ShapeDtypeStruct((rows, padded), BF16),
            compiler_params=params(8),
            cost_estimate=pl.CostEstimate(
                flops=2 * rows * deep * ranks * len(blocks),
                bytes_accessed=2 * deep * ranks * len(blocks),
                transcendentals=0,
            ),
            name="inner",
        )(jnp.stack(places).astype(jnp.int32), normed, *blocks)
    total = jnp.zeros((rows, ranks), F32)
    for place, block in zip(places, blocks):
        own = lax.dynamic_slice_in_dim(normed, place * deep, deep, 1)
        total += jnp.dot(own, block.T, preferred_element_type=F32)
    return jnp.pad(total, ((0, 0), (0, padded - ranks))).astype(BF16)


def assemble_kernel(order_ref, *refs, widths, count):
    blocks, outs = refs[:count], refs[count:]
    offset = 0
    for width, out_ref in zip(widths, outs):
        total = out_ref.shape[1]
        if width % 128 == 0:
            for j, block in enumerate(blocks):
                at = pl.multiple_of(order_ref[j] * width, 128)
                out_ref[:, pl.ds(at, width)] = block[:, offset : offset + width]
        else:
            placed = jnp.zeros((out_ref.shape[0], total), F32)
            source = lax.broadcasted_iota(jnp.int32, (width, total), 0)
            target = lax.broadcasted_iota(jnp.int32, (width, total), 1)
            for j, block in enumerate(blocks):
                chosen = (target == source + order_ref[j] * width).astype(BF16)
                placed += jnp.dot(
                    block[:, offset : offset + width], chosen, preferred_element_type=F32
                )
            out_ref[...] = placed.astype(BF16)
        offset += width


def assemble(blocks, order, widths):
    rank = blocks[0].shape[0]
    count = len(blocks)
    return pl.pallas_call(
        functools.partial(assemble_kernel, widths=widths, count=count),
        grid_spec=pltpu.PrefetchScalarGridSpec(
            num_scalar_prefetch=1,
            grid=(1,),
            in_specs=[whole(b.shape) for b in blocks],
            out_specs=[whole((rank, w * count)) for w in widths],
        ),
        out_shape=[jax.ShapeDtypeStruct((rank, w * count), BF16) for w in widths],
        compiler_params=params(8),
        name="assemble",
    )(jnp.stack(order).astype(jnp.int32), *blocks)


def attend_kernel(
    lengths_ref, q_ref, kv_ref, q_up, k_up, v_up, od_ref, cos_ref, sin_ref, *refs,
    parts, group, block, far,
):
    parts_refs = refs[:parts]
    keys_hbm, values_hbm, w_hbm, ctx_ref, pm_ref, out_ref = refs[parts : parts + 6]
    keys, values, weights, qs, nk, nv, cs, key_sems, value_sems, w_sems = refs[parts + 6 :]
    rows, dim = cos_ref.shape
    heads = q_ref.shape[1] // dim
    kv = heads // group
    rank = q_up.shape[0]
    scale = 1.0 / math.sqrt(dim)
    count = rows // block
    wide = weights.shape[0] * weights.shape[2]

    def cache_copy(source, target, sems, i):
        part = pl.ds(i * block, block)
        return pltpu.make_async_copy(source.at[part], target.at[part], sems.at[i])

    column = exchange(lax.axis_size("tp"))(lax.axis_index("tp"), far)
    tiles, _, size = weights.shape

    def w_copy(n):
        lane = pl.multiple_of(column * wide + n * size, size)
        return pltpu.make_async_copy(w_hbm.at[:, pl.ds(lane, size)], weights.at[n], w_sems.at[n])

    lead = min(2, count)
    for i in range(lead):
        cache_copy(keys_hbm, keys, key_sems, i).start()
        cache_copy(values_hbm, values, value_sems, i).start()

    total = parts_refs[0][...].astype(F32)
    for other in parts_refs[1:]:
        total += other[...].astype(F32)
    inner = total.astype(BF16)
    cosine, sine = cos_ref[...], sin_ref[...]

    def turned(x):
        return x * cosine + pltpu.roll(x, dim // 2, 1) * sine

    def delta(j, up):
        return adapter_scale * jnp.dot(
            inner[:, j * rank : (j + 1) * rank], up[...], preferred_element_type=F32
        )

    key_delta, value_delta, query_delta = delta(1, k_up), delta(2, v_up), delta(0, q_up)
    for g in range(kv):
        lane = slice(g * dim, (g + 1) * dim)
        key = turned(kv_ref[0, :, lane] + key_delta[:, lane]).astype(BF16).astype(F32)
        value = (kv_ref[1, :, lane] + value_delta[:, lane]).astype(BF16).astype(F32)
        for h in range(g * group, (g + 1) * group):
            lane = slice(h * dim, (h + 1) * dim)
            strided = pl.ds(h, rows, stride=heads)
            qs[strided, :] = turned(q_ref[:, lane] + query_delta[:, lane])
            nk[strided, :] = key
            nv[strided, :] = value

    row = lax.broadcasted_iota(jnp.int32, (heads, dim), 0)
    positions = keys.shape[2]
    spot = lax.broadcasted_iota(jnp.int32, (heads, positions), 1)

    def select(pieces):
        out = pieces[0]
        for g in range(1, kv):
            out = jnp.where(row >= g * group, pieces[g], out)
        return out

    def step(i, _):
        @pl.when(i + lead < count)
        def _():
            cache_copy(keys_hbm, keys, key_sems, i + lead).start()
            cache_copy(values_hbm, values, value_sems, i + lead).start()

        @pl.when(i + lead >= count)
        def _():
            for n in range(tiles):
                @pl.when(n * lead // tiles == i + lead - count)
                def _():
                    w_copy(n).start()

        cache_copy(keys_hbm, keys, key_sems, i).wait()
        span = pl.ds(pl.multiple_of(i * block * heads, block * heads), block * heads)
        query = qs[span, :]
        high = query.astype(BF16)
        rest = query - high.astype(F32)
        mid = rest.astype(BF16)
        low = (rest - mid.astype(F32)).astype(BF16)
        found = []
        for b in range(block):
            s = i * block + b
            at = slice(b * heads, (b + 1) * heads)
            q = jnp.concatenate([high[at], mid[at], low[at]], axis=0)
            pieces = []
            for g in range(kv):
                full = lax.dot_general(
                    q, keys[s, g], (((1,), (1,)), ((), ())), preferred_element_type=F32
                )
                pieces.append(full[:heads] + (full[heads : 2 * heads] + full[2 * heads :]))
            found.append(jnp.where(spot < lengths_ref[s], select(pieces) * scale, -1e30))
        scores = jnp.concatenate(found, axis=0)
        own_score = jnp.sum(query * nk[span, :], axis=-1, keepdims=True) * scale
        top = jnp.maximum(jnp.max(scores, axis=-1, keepdims=True), own_score)
        exps = jnp.exp(scores - top)
        own_weight = jnp.exp(own_score - top)
        denom = jnp.sum(exps, axis=-1, keepdims=True) + own_weight
        inverse = 1.0 / denom
        probs = (exps * inverse).astype(BF16)
        own_prob = (own_weight * inverse).astype(BF16).astype(F32)
        cache_copy(values_hbm, values, value_sems, i).wait()
        found = []
        for b in range(block):
            s = i * block + b
            p = probs[b * heads : (b + 1) * heads]
            pieces = [
                jnp.dot(p, values[s, g], preferred_element_type=F32) for g in range(kv)
            ]
            found.append(select(pieces))
        cs[span, :] = jnp.concatenate(found, axis=0) + own_prob * nv[span, :]
        return 0

    lax.fori_loop(0, count, step, 0)

    middle = jnp.zeros((rows, rank), F32)
    for h in range(heads):
        lane = slice(h * dim, (h + 1) * dim)
        context = cs[pl.ds(h, rows, stride=heads), :].astype(BF16)
        ctx_ref[:, lane] = context
        middle += lax.dot_general(
            context, od_ref[:, lane], (((1,), (1,)), ((), ())), preferred_element_type=F32
        )
    high = middle.astype(BF16)
    low = (middle - high.astype(F32)).astype(BF16)
    tail = jnp.concatenate([high, low], axis=1)
    pm_ref[...] = tail

    def project(n, _):
        w_copy(n).wait()
        lane = pl.ds(pl.multiple_of(n * size, size), size)
        part = jnp.dot(ctx_ref[...], weights[n], preferred_element_type=F32)
        out_ref[:, lane] = part.astype(BF16)
        return 0

    lax.fori_loop(0, tiles, project, 0)
    out_ref[:, wide:] = tail


def attention(lengths, base_q, base_kv, parts, ups, od, angles, keys, values, weights, far):
    rows, kv, positions, dim = keys.shape
    q_cols = base_q.shape[1]
    heads = q_cols // dim
    rank = od.shape[0]
    block = 16 if rows % 16 == 0 else rows
    wide = weights.shape[1] // lax.axis_size("tp")
    size = 512 if wide % 512 == 0 else wide
    vmem = pl.BlockSpec(memory_space=pltpu.VMEM)
    hbm = pl.BlockSpec(memory_space=pltpu.HBM)
    fixed = [base_q, base_kv] + list(ups) + [od] + list(angles) + list(parts)
    scratch = pltpu.VMEM((rows * heads, dim), F32)
    return pl.pallas_call(
        functools.partial(
            attend_kernel, parts=len(parts), group=heads // kv, block=block, far=far
        ),
        in_specs=[pl.BlockSpec(memory_space=pltpu.SMEM)] + [vmem] * len(fixed) + [hbm] * 3,
        out_specs=[vmem, vmem, vmem],
        scratch_shapes=[
            pltpu.VMEM(keys.shape, BF16),
            pltpu.VMEM(values.shape, BF16),
            pltpu.VMEM((wide // size, weights.shape[0], size), BF16),
            scratch,
            scratch,
            scratch,
            scratch,
            pltpu.SemaphoreType.DMA((rows // block,)),
            pltpu.SemaphoreType.DMA((rows // block,)),
            pltpu.SemaphoreType.DMA((wide // size,)),
        ],
        out_shape=[
            jax.ShapeDtypeStruct((rows, q_cols), BF16),
            jax.ShapeDtypeStruct((rows, 2 * rank), BF16),
            jax.ShapeDtypeStruct((rows, wide + 2 * rank), BF16),
        ],
        compiler_params=params(52),
        cost_estimate=pl.CostEstimate(
            flops=4 * rows * heads * positions * dim * 16,
            bytes_accessed=4 * keys.size,
            transcendentals=rows * heads * positions,
        ),
        name="attend",
    )(lengths, *fixed, keys, values, weights)


def chunk_kernel(ctx_ref, w_hbm, pm_ref, out_ref, held, sems, *, k):
    tiles, _, size = held.shape
    wide = tiles * size
    column = exchange(lax.axis_size("tp"))(lax.axis_index("tp"), k)

    def copy(n):
        lane = pl.multiple_of(column * wide + n * size, size)
        return pltpu.make_async_copy(w_hbm.at[:, pl.ds(lane, size)], held.at[n], sems.at[n])

    for n in range(tiles):
        copy(n).start()

    def project(n, _):
        copy(n).wait()
        lane = pl.ds(pl.multiple_of(n * size, size), size)
        part = jnp.dot(ctx_ref[...], held[n], preferred_element_type=F32)
        out_ref[:, lane] = part.astype(out_ref.dtype)
        return 0

    lax.fori_loop(0, tiles, project, 0)
    if k:
        out_ref[:, wide:] = pm_ref[...]


def chunk(context, weights, middle, k):
    rows, depth = context.shape
    wide = weights.shape[1] // lax.axis_size("tp")
    size = 512 if wide % 512 == 0 else wide
    tail = middle.shape[1] if k else 0
    vmem = pl.BlockSpec(memory_space=pltpu.VMEM)
    return pl.pallas_call(
        functools.partial(chunk_kernel, k=k),
        in_specs=[vmem, pl.BlockSpec(memory_space=pltpu.HBM), vmem],
        out_specs=vmem,
        out_shape=jax.ShapeDtypeStruct((rows, wide + tail), BF16 if k else F32),
        scratch_shapes=[
            pltpu.VMEM((wide // size, depth, size), BF16),
            pltpu.SemaphoreType.DMA((wide // size,)),
        ],
        compiler_params=params(52),
        cost_estimate=pl.CostEstimate(
            flops=2 * rows * depth * wide, bytes_accessed=2 * depth * wide, transcendentals=0
        ),
    )(context, weights, middle)


def final_kernel(own_ref, pm_ref, up_ref, *refs):
    others, out_ref = refs[:-1], refs[-1]
    wide = own_ref.shape[1]
    rank = up_ref.shape[0]
    total = own_ref[...]
    middle = pm_ref[:, :rank].astype(F32) + pm_ref[:, rank:].astype(F32)
    for other in others:
        total += other[:, :wide].astype(F32)
        tail = other[:, wide:].astype(F32)
        middle += tail[:, :rank] + tail[:, rank:]
    total += adapter_scale * jnp.dot(
        middle.astype(BF16), up_ref[...], preferred_element_type=F32
    )
    out_ref[...] = total.astype(BF16)


def finish(own, middle, out_up, others):
    args = [own, middle, out_up] + others
    return pl.pallas_call(
        final_kernel,
        grid=(1,),
        in_specs=[whole(a.shape) for a in args],
        out_specs=whole(own.shape),
        out_shape=jax.ShapeDtypeStruct(own.shape, BF16),
        compiler_params=params(8),
        name="final",
    )(*args)


def local(
    hidden,
    norm_gain,
    query_weight_matrix,
    key_value_weight,
    output_weight_matrix,
    input_down_factors,
    query_up_factor,
    key_value_up_factors,
    output_down_factor,
    output_up_factor,
    cache_keys,
    cache_values,
    lengths,
):
    rep = lax.axis_size("rep")
    tp = lax.axis_size("tp")
    t = lax.axis_index("tp")

    head_dim = cache_keys.shape[3]
    count, deep, rank = input_down_factors.shape
    down = input_down_factors.transpose(0, 2, 1).reshape(count * rank, deep)
    down_blocks, down_order = gather_rep(down)
    up_pack, widths = pack(
        query_up_factor, output_down_factor, output_up_factor, key_value_up_factors
    )
    moved = lax.ppermute(
        up_pack, ("rep", "tp"), [(b, (b % rep) * tp + b // rep) for b in range(rep * tp)]
    )
    normed, cosine, sine, base_q, base_kv = base_projections(
        hidden, norm_gain, lengths, query_weight_matrix, key_value_weight, head_dim
    )
    moved, base_q = lax.optimization_barrier((moved, base_q))
    up_blocks, up_order = gather_rep(moved)
    part = partial_inner(normed, down_blocks, [o * tp + t for o in down_order])
    parts = [part] + [hop(part, "tp", k) for k in range(1, tp)]
    q_up, od, out_up, k_up, v_up = assemble(up_blocks, up_order, widths)
    far = tp - 1
    context, middle, piece = attention(
        lengths, base_q, base_kv, parts, (q_up, k_up, v_up), od, (cosine, sine),
        cache_keys, cache_values, output_weight_matrix, far,
    )
    others = [hop(piece, "tp", far)]
    for k in range(far - 1, 0, -1):
        piece = chunk(context, output_weight_matrix, middle, k)
        others.append(hop(piece, "tp", k))
    own = chunk(context, output_weight_matrix, middle, 0)
    return finish(own, middle, out_up, others)


def solution(mesh):
    return jax.shard_map(
        local,
        mesh=mesh,
        in_specs=(
            P("rep", None),
            P(),
            P(None, "tp"),
            P(None, None, "tp"),
            P("tp", None),
            P(None, ("rep", "tp"), None),
            P(None, ("rep", "tp")),
            P(None, None, ("rep", "tp")),
            P(("rep", "tp"), None),
            P(None, ("rep", "tp")),
            P("rep", "tp", None, None),
            P("rep", "tp", None, None),
            P("rep"),
        ),
        out_specs=P("rep", "tp"),
        check_vma=False,
    )
```

```python
import functools
import math

import jax
import jax.numpy as jnp
from jax import lax
from jax.experimental import pallas as pl
from jax.experimental.pallas import tpu as pltpu
from jax.sharding import PartitionSpec as P


epsilon = 1e-06
rope_base = 1000000.0
adapter_scale = 0.5
F32 = jnp.float32
BF16 = jnp.bfloat16


INNER = 6 * 10**9
LONG = pl.CostEstimate(flops=1 << 34, bytes_accessed=1 << 20, transcendentals=0)


def params(mib=24):
    return pltpu.CompilerParams(vmem_limit_bytes=mib * 1024 * 1024)


def whole(shape):
    return pl.BlockSpec(shape, lambda *_: (0,) * len(shape))


def power_of_two(n):
    return n & (n - 1) == 0


def exchange(n):
    if power_of_two(n):
        return lambda i, k: i ^ k
    return lambda i, k: (i + k) % n


def hop(x, axis, k):
    n = lax.axis_size(axis)
    to = exchange(n)
    return lax.ppermute(x, axis, [(i, to(i, k)) for i in range(n)])


def came_from(index, n, k):
    if power_of_two(n):
        return index ^ k
    return (index - k) % n


def gather_rep(block):
    n = lax.axis_size("rep")

    def sent(x, k):
        return hop(x, "rep", k)

    if not power_of_two(n) or n == 1:
        return [block] + [sent(block, k) for k in range(1, n)]
    near = [block] + [sent(block, k) for k in range(2, n, 2)]
    swapped = []
    for b in near:
        swapped.append(hop(b, "rep", 1))
    return near + swapped


def rep_order():
    n = lax.axis_size("rep")
    r = lax.axis_index("rep")
    if not power_of_two(n) or n == 1:
        return [came_from(r, n, k) for k in range(n)]
    return [r ^ k for k in range(0, n, 2)] + [r ^ k ^ 1 for k in range(0, n, 2)]


def pack_kernel(q_ref, od_ref, ou_ref, kv_ref, out_ref):
    both = jnp.concatenate([kv_ref[0], kv_ref[1]], axis=0).astype(F32).T.astype(BF16)
    lane = 0
    for piece in (q_ref[...], od_ref[...], ou_ref[...], both):
        out_ref[:, lane : lane + piece.shape[1]] = piece
        lane += piece.shape[1]


def pack(q_up, od, ou, kv_up):
    widths = (q_up.shape[1], od.shape[0], ou.shape[1], kv_up.shape[2], kv_up.shape[2])
    if any(w % 128 for w in widths[:3]):
        return jnp.concatenate([q_up, od.T, ou, kv_up[0], kv_up[1]], axis=1), widths
    vmem = pl.BlockSpec(memory_space=pltpu.VMEM)
    packed = pl.pallas_call(
        pack_kernel,
        in_specs=[vmem] * 4,
        out_specs=vmem,
        out_shape=jax.ShapeDtypeStruct((q_up.shape[0], sum(widths)), BF16),
        compiler_params=params(4),
        name="pack",
    )(q_up, od.T, ou, kv_up.transpose(0, 2, 1))
    return packed, widths


def opening_kernel(out_ref):
    out_ref[...] = jnp.zeros_like(out_ref)


def opening():
    return pl.pallas_call(
        opening_kernel,
        out_specs=pl.BlockSpec(memory_space=pltpu.VMEM),
        out_shape=jax.ShapeDtypeStruct((8, 128), F32),
        compiler_params=params(1),
        cost_estimate=LONG,
        name="opening",
    )()


def tables_kernel(lengths_ref, _, cos_ref, sin_ref, angle):
    rows = cos_ref.shape[0]
    dim = cos_ref.shape[1]
    spot = lax.broadcasted_iota(jnp.int32, (1, dim), 1) % (dim // 2)
    freq = jnp.ones((1, dim), F32)
    for bit in range((dim // 2 - 1).bit_length()):
        power = rope_base ** (-(2.0 ** (bit + 1)) / dim)
        freq *= jnp.where((spot >> bit) % 2 == 1, power, 1.0)
    for s in range(rows):
        angle[s : s + 1, :] = freq * lengths_ref[s].astype(F32)
    low = lax.broadcasted_iota(jnp.int32, (rows, dim), 1) < dim // 2
    wave = jnp.sin(angle[...] + jnp.where(low, 0.0, math.pi / 2))
    other = pltpu.roll(wave, dim // 2, 1)
    cos_ref[...] = jnp.where(low, other, wave)
    sin_ref[...] = jnp.where(low, -wave, other)


def tables(lengths, opened, dim):
    rows = lengths.shape[0]
    vmem = pl.BlockSpec(memory_space=pltpu.VMEM)
    return pl.pallas_call(
        tables_kernel,
        in_specs=[pl.BlockSpec(memory_space=pltpu.SMEM), vmem],
        out_specs=[vmem] * 2,
        out_shape=[jax.ShapeDtypeStruct((rows, dim), F32)] * 2,
        scratch_shapes=[pltpu.VMEM((rows, dim), F32)],
        compiler_params=params(4),
        name="tables",
    )(lengths, opened)


def base_kernel(gain_ref, hidden, q_held, kv_held, x_ref, q_out, kv_out):
    rows, wide = hidden.shape
    depth = 512

    q_out[...] = jnp.zeros_like(q_out)
    kv_out[...] = jnp.zeros_like(kv_out)

    part = gain_ref.shape[1]
    square = jnp.zeros((rows, part), F32)
    for j in range(wide // part):
        states = hidden[:, j * part : (j + 1) * part].astype(F32)
        square += states * states
    factor = lax.rsqrt(jnp.sum(square, axis=-1, keepdims=True) / wide + epsilon)
    for j in range(wide // part):
        lane = slice(j * part, (j + 1) * part)
        scaled = hidden[:, lane].astype(F32) * factor * gain_ref[j : j + 1, :].astype(F32)
        x_ref[:, lane] = scaled.astype(BF16)

    def step(i, _):
        rows_at = pl.ds(pl.multiple_of(i * depth, depth), depth)
        x = x_ref[:, rows_at]
        q_out[...] += jnp.dot(x, q_held[rows_at, :], preferred_element_type=F32)
        for j in range(kv_held.shape[0]):
            kv_out[j] += jnp.dot(x, kv_held[j, rows_at, :], preferred_element_type=F32)
        return 0

    lax.fori_loop(0, wide // depth, step, 0)


def base_projections(hidden, gain, q_weights, kv_weights):
    rows, wide = hidden.shape
    q_cols, kv_cols = q_weights.shape[1], kv_weights.shape[2]
    pair = kv_weights.shape[0]
    vmem = pl.BlockSpec(memory_space=pltpu.VMEM)
    return pl.pallas_call(
        base_kernel,
        in_specs=[vmem] * 4,
        out_specs=[vmem] * 3,
        out_shape=[
            jax.ShapeDtypeStruct((rows, wide), BF16),
            jax.ShapeDtypeStruct((rows, q_cols), F32),
            jax.ShapeDtypeStruct((pair, rows, kv_cols), F32),
        ],
        compiler_params=params(6),
        cost_estimate=pl.CostEstimate(
            flops=16 * rows * (q_weights.size + kv_weights.size),
            bytes_accessed=2 * (q_weights.size + kv_weights.size),
            transcendentals=0,
        ),
        name="base",
    )(gain.reshape(wide // 128, 128), hidden, q_weights, kv_weights)


def inner_kernel(x_ref, *refs):
    blocks, out_ref = refs[:-1], refs[-1]
    order = rep_order()
    tp, t = lax.axis_size("tp"), lax.axis_index("tp")
    ranks, deep = blocks[0].shape
    total = jnp.zeros((x_ref.shape[0], ranks), F32)
    for j, block in enumerate(blocks):
        at = pl.multiple_of((order[j] * tp + t) * deep, deep)
        total += lax.dot_general(
            x_ref[:, pl.ds(at, deep)],
            block[...],
            (((1,), (1,)), ((), ())),
            preferred_element_type=F32,
        )
    rest = jnp.zeros((x_ref.shape[0], out_ref.shape[1] - ranks), F32)
    out_ref[...] = jnp.concatenate([total, rest], axis=1).astype(BF16)


def partial_inner(normed, blocks):
    ranks, deep = blocks[0].shape
    rows = normed.shape[0]
    padded = -(-ranks // 128) * 128
    vmem = pl.BlockSpec(memory_space=pltpu.VMEM)
    if deep % 128 == 0:
        return pl.pallas_call(
            inner_kernel,
            in_specs=[vmem] * (1 + len(blocks)),
            out_specs=vmem,
            out_shape=jax.ShapeDtypeStruct((rows, padded), BF16),
            compiler_params=params(4),
            cost_estimate=pl.CostEstimate(flops=INNER, bytes_accessed=1 << 20, transcendentals=0),
            name="inner",
        )(normed, *blocks)
    total = jnp.zeros((rows, ranks), F32)
    tp, t = lax.axis_size("tp"), lax.axis_index("tp")
    for place, block in zip(rep_order(), blocks):
        place = place * tp + t
        own = lax.dynamic_slice_in_dim(normed, place * deep, deep, 1)
        total += jnp.dot(own, block.T, preferred_element_type=F32)
    return jnp.pad(total, ((0, 0), (0, padded - ranks))).astype(BF16)


def assemble_kernel(*refs, widths, count):
    blocks, outs = refs[:count], refs[count:]
    order = rep_order()
    offset = 0
    for width, out_ref in zip(widths, outs):
        total = out_ref.shape[1]
        if width % 128 == 0:
            for j, block in enumerate(blocks):
                at = pl.multiple_of(order[j] * width, 128)
                out_ref[:, pl.ds(at, width)] = block[:, offset : offset + width]
        else:
            placed = jnp.zeros((out_ref.shape[0], total), F32)
            source = lax.broadcasted_iota(jnp.int32, (width, total), 0)
            target = lax.broadcasted_iota(jnp.int32, (width, total), 1)
            for j, block in enumerate(blocks):
                chosen = (target == source + order[j] * width).astype(BF16)
                placed += jnp.dot(
                    block[:, offset : offset + width], chosen, preferred_element_type=F32
                )
            out_ref[...] = placed.astype(BF16)
        offset += width


def assemble(blocks, widths):
    rank = blocks[0].shape[0]
    count = len(blocks)
    vmem = pl.BlockSpec(memory_space=pltpu.VMEM)
    return pl.pallas_call(
        functools.partial(assemble_kernel, widths=widths, count=count),
        in_specs=[vmem] * count,
        out_specs=[vmem] * len(widths),
        out_shape=[jax.ShapeDtypeStruct((rank, w * count), BF16) for w in widths],
        compiler_params=params(4),
        name="assemble",
    )(*blocks)


def attend_kernel(
    lengths_ref, q_ref, kv_ref, q_up, k_up, v_up, od_ref, cos_ref, sin_ref, *refs,
    parts, group, block, far,
):
    parts_refs = refs[:parts]
    keys, values, weights, ctx_ref, pm_ref, out_ref = refs[parts : parts + 6]
    qs, nk, nv, cs = refs[parts + 6 :]
    rows, dim = cos_ref.shape
    heads = q_ref.shape[1] // dim
    kv = heads // group
    rank = q_up.shape[0]
    scale = 1.0 / math.sqrt(dim)
    count = rows // block
    wide = out_ref.shape[1] - pm_ref.shape[1]
    size = 512 if wide % 512 == 0 else wide
    column = exchange(lax.axis_size("tp"))(lax.axis_index("tp"), far) * wide

    total = parts_refs[0][...].astype(F32)
    for other in parts_refs[1:]:
        total += other[...].astype(F32)
    inner = total.astype(BF16)
    cosine, sine = cos_ref[...], sin_ref[...]

    def turned(x):
        return x * cosine + pltpu.roll(x, dim // 2, 1) * sine

    def delta(j, up):
        return adapter_scale * jnp.dot(
            inner[:, j * rank : (j + 1) * rank], up[...], preferred_element_type=F32
        )

    key_delta, value_delta, query_delta = delta(1, k_up), delta(2, v_up), delta(0, q_up)
    for g in range(kv):
        lane = slice(g * dim, (g + 1) * dim)
        key = turned(kv_ref[0, :, lane] + key_delta[:, lane]).astype(BF16).astype(F32)
        value = (kv_ref[1, :, lane] + value_delta[:, lane]).astype(BF16).astype(F32)
        for h in range(g * group, (g + 1) * group):
            lane = slice(h * dim, (h + 1) * dim)
            strided = pl.ds(h, rows, stride=heads)
            qs[strided, :] = turned(q_ref[:, lane] + query_delta[:, lane])
            nk[strided, :] = key
            nv[strided, :] = value

    row = lax.broadcasted_iota(jnp.int32, (heads, dim), 0)
    positions = keys.shape[2]
    spot = lax.broadcasted_iota(jnp.int32, (heads, positions), 1)

    def select(pieces):
        out = pieces[0]
        for g in range(1, kv):
            out = jnp.where(row >= g * group, pieces[g], out)
        return out

    def step(i, _):
        span = pl.ds(pl.multiple_of(i * block * heads, block * heads), block * heads)
        query = qs[span, :]
        high = query.astype(BF16)
        rest = query - high.astype(F32)
        mid = rest.astype(BF16)
        low = (rest - mid.astype(F32)).astype(BF16)
        found = []
        for b in range(block):
            s = i * block + b
            at = slice(b * heads, (b + 1) * heads)
            q = jnp.concatenate([high[at], mid[at], low[at]], axis=0)
            pieces = []
            for g in range(kv):
                full = lax.dot_general(
                    q, keys[s, g], (((1,), (1,)), ((), ())), preferred_element_type=F32
                )
                pieces.append(full[:heads] + (full[heads : 2 * heads] + full[2 * heads :]))
            found.append(jnp.where(spot < lengths_ref[s], select(pieces) * scale, -1e30))
        scores = jnp.concatenate(found, axis=0)
        own_score = jnp.sum(query * nk[span, :], axis=-1, keepdims=True) * scale
        top = jnp.maximum(jnp.max(scores, axis=-1, keepdims=True), own_score)
        exps = jnp.exp(scores - top)
        own_weight = jnp.exp(own_score - top)
        denom = jnp.sum(exps, axis=-1, keepdims=True) + own_weight
        inverse = 1.0 / denom
        probs = (exps * inverse).astype(BF16)
        own_prob = (own_weight * inverse).astype(BF16).astype(F32)
        found = []
        for b in range(block):
            s = i * block + b
            p = probs[b * heads : (b + 1) * heads]
            pieces = [
                jnp.dot(p, values[s, g], preferred_element_type=F32) for g in range(kv)
            ]
            found.append(select(pieces))
        cs[span, :] = jnp.concatenate(found, axis=0) + own_prob * nv[span, :]
        return 0

    lax.fori_loop(0, count, step, 0)

    middle = jnp.zeros((rows, rank), F32)
    for h in range(heads):
        lane = slice(h * dim, (h + 1) * dim)
        context = cs[pl.ds(h, rows, stride=heads), :].astype(BF16)
        ctx_ref[:, lane] = context
        middle += lax.dot_general(
            context, od_ref[:, lane], (((1,), (1,)), ((), ())), preferred_element_type=F32
        )
    high = middle.astype(BF16)
    low = (middle - high.astype(F32)).astype(BF16)
    tail = jnp.concatenate([high, low], axis=1)
    pm_ref[...] = tail

    def project(n, _):
        lane = pl.ds(pl.multiple_of(n * size, size), size)
        at = pl.ds(pl.multiple_of(column + n * size, size), size)
        part = jnp.dot(ctx_ref[...], weights[:, at], preferred_element_type=F32)
        out_ref[:, lane] = part.astype(BF16)
        return 0

    lax.fori_loop(0, wide // size, project, 0)
    out_ref[:, wide:] = tail


def attention(lengths, base_q, base_kv, parts, ups, od, angles, keys, values, weights, far):
    rows, kv, positions, dim = keys.shape
    q_cols = base_q.shape[1]
    heads = q_cols // dim
    rank = od.shape[0]
    block = 16 if rows % 16 == 0 else rows
    wide = weights.shape[1] // lax.axis_size("tp")
    vmem = pl.BlockSpec(memory_space=pltpu.VMEM)
    fixed = [base_q, base_kv] + list(ups) + [od] + list(angles) + list(parts)
    scratch = pltpu.VMEM((rows * heads, dim), F32)
    return pl.pallas_call(
        functools.partial(
            attend_kernel, parts=len(parts), group=heads // kv, block=block, far=far
        ),
        in_specs=[pl.BlockSpec(memory_space=pltpu.SMEM)] + [vmem] * (len(fixed) + 3),
        out_specs=[vmem, vmem, vmem],
        scratch_shapes=[
            scratch,
            scratch,
            scratch,
            scratch,
        ],
        out_shape=[
            jax.ShapeDtypeStruct((rows, q_cols), BF16),
            jax.ShapeDtypeStruct((rows, 2 * rank), BF16),
            jax.ShapeDtypeStruct((rows, wide + 2 * rank), BF16),
        ],
        compiler_params=params(8),
        cost_estimate=pl.CostEstimate(
            flops=4 * rows * heads * positions * dim * 16,
            bytes_accessed=4 * keys.size,
            transcendentals=rows * heads * positions,
        ),
        name="attend",
    )(lengths, *fixed, keys, values, weights)


def chunk_kernel(ctx_ref, w_ref, pm_ref, out_ref, *, k):
    wide = out_ref.shape[1] - (pm_ref.shape[1] if k else 0)
    size = 512 if wide % 512 == 0 else wide
    column = exchange(lax.axis_size("tp"))(lax.axis_index("tp"), k) * wide

    def project(n, _):
        lane = pl.ds(pl.multiple_of(n * size, size), size)
        at = pl.ds(pl.multiple_of(column + n * size, size), size)
        part = jnp.dot(ctx_ref[...], w_ref[:, at], preferred_element_type=F32)
        out_ref[:, lane] = part.astype(out_ref.dtype)
        return 0

    lax.fori_loop(0, wide // size, project, 0)
    if k:
        out_ref[:, wide:] = pm_ref[...]


def chunk(context, weights, middle, k):
    rows, depth = context.shape
    wide = weights.shape[1] // lax.axis_size("tp")
    tail = middle.shape[1] if k else 0
    vmem = pl.BlockSpec(memory_space=pltpu.VMEM)
    return pl.pallas_call(
        functools.partial(chunk_kernel, k=k),
        in_specs=[vmem, vmem, vmem],
        out_specs=vmem,
        out_shape=jax.ShapeDtypeStruct((rows, wide + tail), BF16 if k else F32),
        compiler_params=params(4),
        cost_estimate=pl.CostEstimate(
            flops=2 * rows * depth * wide, bytes_accessed=2 * depth * wide, transcendentals=0
        ),
    )(context, weights, middle)


def final_kernel(own_ref, pm_ref, up_ref, *refs):
    others, out_ref = refs[:-1], refs[-1]
    wide = own_ref.shape[1]
    rank = up_ref.shape[0]
    total = own_ref[...]
    middle = pm_ref[:, :rank].astype(F32) + pm_ref[:, rank:].astype(F32)
    for other in others:
        total += other[:, :wide].astype(F32)
        tail = other[:, wide:].astype(F32)
        middle += tail[:, :rank] + tail[:, rank:]
    total += adapter_scale * jnp.dot(
        middle.astype(BF16), up_ref[...], preferred_element_type=F32
    )
    out_ref[...] = total.astype(BF16)


def finish(own, middle, out_up, others):
    args = [own, middle, out_up] + others
    return pl.pallas_call(
        final_kernel,
        grid=(1,),
        in_specs=[whole(a.shape) for a in args],
        out_specs=whole(own.shape),
        out_shape=jax.ShapeDtypeStruct(own.shape, BF16),
        compiler_params=params(8),
        name="final",
    )(*args)


def local(
    hidden,
    norm_gain,
    query_weight_matrix,
    key_value_weight,
    output_weight_matrix,
    input_down_factors,
    query_up_factor,
    key_value_up_factors,
    output_down_factor,
    output_up_factor,
    cache_keys,
    cache_values,
    lengths,
):
    rep = lax.axis_size("rep")
    tp = lax.axis_size("tp")

    head_dim = cache_keys.shape[3]
    count, deep, rank = input_down_factors.shape
    input_down_factors, opened = lax.optimization_barrier((input_down_factors, opening()))
    cosine, sine = tables(lengths, opened, head_dim)
    down = input_down_factors.transpose(0, 2, 1).reshape(count * rank, deep)
    down_blocks = gather_rep(down)
    up_pack, widths = pack(
        query_up_factor, output_down_factor, output_up_factor, key_value_up_factors
    )
    moved = lax.ppermute(
        up_pack, ("rep", "tp"), [(b, (b % rep) * tp + b // rep) for b in range(rep * tp)]
    )
    normed, base_q, base_kv = base_projections(
        hidden, norm_gain, query_weight_matrix, key_value_weight
    )
    moved, base_q = lax.optimization_barrier((moved, base_q))
    up_blocks = gather_rep(moved)
    part = partial_inner(normed, down_blocks)
    parts = [part]
    for k in range(1, tp):
        parts.append(hop(part, "tp", k))
    q_up, od, out_up, k_up, v_up = assemble(up_blocks, widths)
    far = tp - 1
    context, middle, piece = attention(
        lengths, base_q, base_kv, parts, (q_up, k_up, v_up), od, (cosine, sine),
        cache_keys, cache_values, output_weight_matrix, far,
    )
    others = [hop(piece, "tp", far)]
    for k in range(far - 1, 0, -1):
        piece = chunk(context, output_weight_matrix, middle, k)
        others.append(hop(piece, "tp", k))
    own = chunk(context, output_weight_matrix, middle, 0)
    return finish(own, middle, out_up, others)


def solution(mesh):
    return jax.shard_map(
        local,
        mesh=mesh,
        in_specs=(
            P("rep", None),
            P(),
            P(None, "tp"),
            P(None, None, "tp"),
            P("tp", None),
            P(None, ("rep", "tp"), None),
            P(None, ("rep", "tp")),
            P(None, None, ("rep", "tp")),
            P(("rep", "tp"), None),
            P(None, ("rep", "tp")),
            P("rep", "tp", None, None),
            P("rep", "tp", None, None),
            P("rep"),
        ),
        out_specs=P("rep", "tp"),
        check_vma=False,
    )
```

```python
import functools
import math

import jax
import jax.numpy as jnp
from jax import lax
from jax.experimental import pallas as pl
from jax.experimental.pallas import tpu as pltpu
from jax.sharding import PartitionSpec as P


epsilon = 1e-06
rope_base = 1000000.0
adapter_scale = 0.5
F32 = jnp.float32
BF16 = jnp.bfloat16


INNER = 6 * 10**9
LINE = ((3, 2, 1, 0), (2, 0, 3, 1), (1, 3, 0, 2))
LONG = pl.CostEstimate(flops=1 << 34, bytes_accessed=1 << 20, transcendentals=0)


def params(mib=24):
    return pltpu.CompilerParams(vmem_limit_bytes=mib * 1024 * 1024)


def whole(shape):
    return pl.BlockSpec(shape, lambda *_: (0,) * len(shape))


def power_of_two(n):
    return n & (n - 1) == 0


def exchange(n):
    if power_of_two(n):
        return lambda i, k: i ^ k
    return lambda i, k: (i + k) % n


def hop(x, axis, k):
    n = lax.axis_size(axis)
    to = exchange(n)
    return lax.ppermute(x, axis, [(i, to(i, k)) for i in range(n)])


def came_from(index, n, k):
    if power_of_two(n):
        return index ^ k
    return (index - k) % n


def chunk_target(target):
    t = lax.axis_index("tp")
    if isinstance(target, tuple):
        found = target[0]
        for place in range(1, len(target)):
            found = jnp.where(t == place, target[place], found)
        return found
    return exchange(lax.axis_size("tp"))(t, target)


def gather_rep(block):
    n = lax.axis_size("rep")

    def sent(x, k):
        return hop(x, "rep", k)

    if not power_of_two(n) or n == 1:
        return [block] + [sent(block, k) for k in range(1, n)]
    near = [block] + [sent(block, k) for k in range(2, n, 2)]
    swapped = []
    for b in near:
        swapped.append(hop(b, "rep", 1))
    return near + swapped


def rep_order():
    n = lax.axis_size("rep")
    r = lax.axis_index("rep")
    if not power_of_two(n) or n == 1:
        return [came_from(r, n, k) for k in range(n)]
    return [r ^ k for k in range(0, n, 2)] + [r ^ k ^ 1 for k in range(0, n, 2)]


def pack_kernel(q_ref, od_ref, ou_ref, kv_ref, out_ref):
    both = jnp.concatenate([kv_ref[0], kv_ref[1]], axis=0).astype(F32).T.astype(BF16)
    lane = 0
    for piece in (q_ref[...], od_ref[...], ou_ref[...], both):
        out_ref[:, lane : lane + piece.shape[1]] = piece
        lane += piece.shape[1]


def pack(q_up, od, ou, kv_up):
    widths = (q_up.shape[1], od.shape[0], ou.shape[1], kv_up.shape[2], kv_up.shape[2])
    if any(w % 128 for w in widths[:3]):
        return jnp.concatenate([q_up, od.T, ou, kv_up[0], kv_up[1]], axis=1), widths
    vmem = pl.BlockSpec(memory_space=pltpu.VMEM)
    packed = pl.pallas_call(
        pack_kernel,
        in_specs=[vmem] * 4,
        out_specs=vmem,
        out_shape=jax.ShapeDtypeStruct((q_up.shape[0], sum(widths)), BF16),
        compiler_params=params(4),
        name="pack",
    )(q_up, od.T, ou, kv_up.transpose(0, 2, 1))
    return packed, widths


def opening_kernel(out_ref):
    out_ref[...] = jnp.zeros_like(out_ref)


def opening():
    return pl.pallas_call(
        opening_kernel,
        out_specs=pl.BlockSpec(memory_space=pltpu.VMEM),
        out_shape=jax.ShapeDtypeStruct((8, 128), F32),
        compiler_params=params(1),
        cost_estimate=LONG,
        name="opening",
    )()


def tables_kernel(lengths_ref, _, cos_ref, sin_ref, angle):
    rows = cos_ref.shape[0]
    dim = cos_ref.shape[1]
    spot = lax.broadcasted_iota(jnp.int32, (1, dim), 1) % (dim // 2)
    freq = jnp.ones((1, dim), F32)
    for bit in range((dim // 2 - 1).bit_length()):
        power = rope_base ** (-(2.0 ** (bit + 1)) / dim)
        freq *= jnp.where((spot >> bit) % 2 == 1, power, 1.0)
    for s in range(rows):
        angle[s : s + 1, :] = freq * lengths_ref[s].astype(F32)
    low = lax.broadcasted_iota(jnp.int32, (rows, dim), 1) < dim // 2
    wave = jnp.sin(angle[...] + jnp.where(low, 0.0, math.pi / 2))
    other = pltpu.roll(wave, dim // 2, 1)
    cos_ref[...] = jnp.where(low, other, wave)
    sin_ref[...] = jnp.where(low, -wave, other)


def tables(lengths, opened, dim):
    rows = lengths.shape[0]
    vmem = pl.BlockSpec(memory_space=pltpu.VMEM)
    return pl.pallas_call(
        tables_kernel,
        in_specs=[pl.BlockSpec(memory_space=pltpu.SMEM), vmem],
        out_specs=[vmem] * 2,
        out_shape=[jax.ShapeDtypeStruct((rows, dim), F32)] * 2,
        scratch_shapes=[pltpu.VMEM((rows, dim), F32)],
        compiler_params=params(4),
        name="tables",
    )(lengths, opened)


def base_kernel(gain_ref, hidden, q_held, kv_held, x_ref, q_out, kv_out):
    rows, wide = hidden.shape
    depth = 512

    q_out[...] = jnp.zeros_like(q_out)
    kv_out[...] = jnp.zeros_like(kv_out)

    part = gain_ref.shape[1]
    square = jnp.zeros((rows, part), F32)
    for j in range(wide // part):
        states = hidden[:, j * part : (j + 1) * part].astype(F32)
        square += states * states
    factor = lax.rsqrt(jnp.sum(square, axis=-1, keepdims=True) / wide + epsilon)
    for j in range(wide // part):
        lane = slice(j * part, (j + 1) * part)
        scaled = hidden[:, lane].astype(F32) * factor * gain_ref[j : j + 1, :].astype(F32)
        x_ref[:, lane] = scaled.astype(BF16)

    def step(i, _):
        rows_at = pl.ds(pl.multiple_of(i * depth, depth), depth)
        x = x_ref[:, rows_at]
        q_out[...] += jnp.dot(x, q_held[rows_at, :], preferred_element_type=F32)
        for j in range(kv_held.shape[0]):
            kv_out[j] += jnp.dot(x, kv_held[j, rows_at, :], preferred_element_type=F32)
        return 0

    lax.fori_loop(0, wide // depth, step, 0)


def base_projections(hidden, gain, q_weights, kv_weights):
    rows, wide = hidden.shape
    q_cols, kv_cols = q_weights.shape[1], kv_weights.shape[2]
    pair = kv_weights.shape[0]
    vmem = pl.BlockSpec(memory_space=pltpu.VMEM)
    return pl.pallas_call(
        base_kernel,
        in_specs=[vmem] * 4,
        out_specs=[vmem] * 3,
        out_shape=[
            jax.ShapeDtypeStruct((rows, wide), BF16),
            jax.ShapeDtypeStruct((rows, q_cols), F32),
            jax.ShapeDtypeStruct((pair, rows, kv_cols), F32),
        ],
        compiler_params=params(6),
        cost_estimate=pl.CostEstimate(
            flops=16 * rows * (q_weights.size + kv_weights.size),
            bytes_accessed=2 * (q_weights.size + kv_weights.size),
            transcendentals=0,
        ),
        name="base",
    )(gain.reshape(wide // 128, 128), hidden, q_weights, kv_weights)


def inner_kernel(x_ref, *refs):
    blocks, out_ref = refs[:-1], refs[-1]
    order = rep_order()
    tp, t = lax.axis_size("tp"), lax.axis_index("tp")
    ranks, deep = blocks[0].shape
    total = jnp.zeros((x_ref.shape[0], ranks), F32)
    for j, block in enumerate(blocks):
        at = pl.multiple_of((order[j] * tp + t) * deep, deep)
        total += lax.dot_general(
            x_ref[:, pl.ds(at, deep)],
            block[...],
            (((1,), (1,)), ((), ())),
            preferred_element_type=F32,
        )
    rest = jnp.zeros((x_ref.shape[0], out_ref.shape[1] - ranks), F32)
    out_ref[...] = jnp.concatenate([total, rest], axis=1).astype(BF16)


def partial_inner(normed, blocks):
    ranks, deep = blocks[0].shape
    rows = normed.shape[0]
    padded = -(-ranks // 128) * 128
    vmem = pl.BlockSpec(memory_space=pltpu.VMEM)
    if deep % 128 == 0:
        return pl.pallas_call(
            inner_kernel,
            in_specs=[vmem] * (1 + len(blocks)),
            out_specs=vmem,
            out_shape=jax.ShapeDtypeStruct((rows, padded), BF16),
            compiler_params=params(4),
            cost_estimate=pl.CostEstimate(flops=INNER, bytes_accessed=1 << 20, transcendentals=0),
            name="inner",
        )(normed, *blocks)
    total = jnp.zeros((rows, ranks), F32)
    tp, t = lax.axis_size("tp"), lax.axis_index("tp")
    for place, block in zip(rep_order(), blocks):
        place = place * tp + t
        own = lax.dynamic_slice_in_dim(normed, place * deep, deep, 1)
        total += jnp.dot(own, block.T, preferred_element_type=F32)
    return jnp.pad(total, ((0, 0), (0, padded - ranks))).astype(BF16)


def assemble_kernel(*refs, widths, count):
    blocks, outs = refs[:count], refs[count:]
    order = rep_order()
    offset = 0
    for width, out_ref in zip(widths, outs):
        total = out_ref.shape[1]
        if width % 128 == 0:
            for j, block in enumerate(blocks):
                at = pl.multiple_of(order[j] * width, 128)
                out_ref[:, pl.ds(at, width)] = block[:, offset : offset + width]
        else:
            placed = jnp.zeros((out_ref.shape[0], total), F32)
            source = lax.broadcasted_iota(jnp.int32, (width, total), 0)
            target = lax.broadcasted_iota(jnp.int32, (width, total), 1)
            for j, block in enumerate(blocks):
                chosen = (target == source + order[j] * width).astype(BF16)
                placed += jnp.dot(
                    block[:, offset : offset + width], chosen, preferred_element_type=F32
                )
            out_ref[...] = placed.astype(BF16)
        offset += width


def assemble(blocks, widths):
    rank = blocks[0].shape[0]
    count = len(blocks)
    vmem = pl.BlockSpec(memory_space=pltpu.VMEM)
    return pl.pallas_call(
        functools.partial(assemble_kernel, widths=widths, count=count),
        in_specs=[vmem] * count,
        out_specs=[vmem] * len(widths),
        out_shape=[jax.ShapeDtypeStruct((rank, w * count), BF16) for w in widths],
        compiler_params=params(4),
        name="assemble",
    )(*blocks)


def attend_kernel(
    lengths_ref, q_ref, kv_ref, q_up, k_up, v_up, od_ref, cos_ref, sin_ref, *refs,
    parts, group, block, far,
):
    parts_refs = refs[:parts]
    keys, values, weights, ctx_ref, pm_ref, out_ref = refs[parts : parts + 6]
    qs, nk, nv, cs = refs[parts + 6 :]
    rows, dim = cos_ref.shape
    heads = q_ref.shape[1] // dim
    kv = heads // group
    rank = q_up.shape[0]
    scale = 1.0 / math.sqrt(dim)
    count = rows // block
    wide = out_ref.shape[1] - pm_ref.shape[1]
    size = 512 if wide % 512 == 0 else wide
    column = chunk_target(far) * wide

    total = parts_refs[0][...].astype(F32)
    for other in parts_refs[1:]:
        total += other[...].astype(F32)
    inner = total.astype(BF16)
    cosine, sine = cos_ref[...], sin_ref[...]

    def turned(x):
        return x * cosine + pltpu.roll(x, dim // 2, 1) * sine

    def delta(j, up):
        return adapter_scale * jnp.dot(
            inner[:, j * rank : (j + 1) * rank], up[...], preferred_element_type=F32
        )

    key_delta, value_delta, query_delta = delta(1, k_up), delta(2, v_up), delta(0, q_up)
    for g in range(kv):
        lane = slice(g * dim, (g + 1) * dim)
        key = turned(kv_ref[0, :, lane] + key_delta[:, lane]).astype(BF16).astype(F32)
        value = (kv_ref[1, :, lane] + value_delta[:, lane]).astype(BF16).astype(F32)
        for h in range(g * group, (g + 1) * group):
            lane = slice(h * dim, (h + 1) * dim)
            strided = pl.ds(h, rows, stride=heads)
            qs[strided, :] = turned(q_ref[:, lane] + query_delta[:, lane])
            nk[strided, :] = key
            nv[strided, :] = value

    row = lax.broadcasted_iota(jnp.int32, (heads, dim), 0)
    positions = keys.shape[2]
    spot = lax.broadcasted_iota(jnp.int32, (heads, positions), 1)

    def select(pieces):
        out = pieces[0]
        for g in range(1, kv):
            out = jnp.where(row >= g * group, pieces[g], out)
        return out

    def score(i):
        span = slice(i * block * heads, (i + 1) * block * heads)
        query = qs[span, :]
        high = query.astype(BF16)
        rest = query - high.astype(F32)
        mid = rest.astype(BF16)
        low = (rest - mid.astype(F32)).astype(BF16)
        found = []
        for b in range(block):
            s = i * block + b
            at = slice(b * heads, (b + 1) * heads)
            q = jnp.concatenate([high[at], mid[at], low[at]], axis=0)
            pieces = []
            for g in range(kv):
                full = lax.dot_general(
                    q, keys[s, g], (((1,), (1,)), ((), ())), preferred_element_type=F32
                )
                pieces.append(full[:heads] + (full[heads : 2 * heads] + full[2 * heads :]))
            found.append(jnp.where(spot < lengths_ref[s], select(pieces) * scale, -1e30))
        own_score = jnp.sum(query * nk[span, :], axis=-1, keepdims=True) * scale
        return jnp.concatenate(found, axis=0), own_score

    def weigh(scores, own_score):
        top = jnp.maximum(jnp.max(scores, axis=-1, keepdims=True), own_score)
        exps = jnp.exp(scores - top)
        own_weight = jnp.exp(own_score - top)
        inverse = 1.0 / (jnp.sum(exps, axis=-1, keepdims=True) + own_weight)
        return (exps * inverse).astype(BF16), (own_weight * inverse).astype(BF16).astype(F32)

    def gather(i, probs, own_prob):
        span = slice(i * block * heads, (i + 1) * block * heads)
        found = []
        for b in range(block):
            s = i * block + b
            p = probs[b * heads : (b + 1) * heads]
            pieces = [
                jnp.dot(p, values[s, g], preferred_element_type=F32) for g in range(kv)
            ]
            found.append(select(pieces))
        cs[span, :] = jnp.concatenate(found, axis=0) + own_prob * nv[span, :]

    scored, weighed = None, None
    for i in range(count + 2):
        if i >= 2:
            gather(i - 2, *weighed)
        if 1 <= i <= count:
            weighed = weigh(*scored)
        if i < count:
            scored = score(i)

    middle = jnp.zeros((rows, rank), F32)
    for h in range(heads):
        lane = slice(h * dim, (h + 1) * dim)
        context = cs[pl.ds(h, rows, stride=heads), :].astype(BF16)
        ctx_ref[:, lane] = context
        middle += lax.dot_general(
            context, od_ref[:, lane], (((1,), (1,)), ((), ())), preferred_element_type=F32
        )
    high = middle.astype(BF16)
    low = (middle - high.astype(F32)).astype(BF16)
    tail = jnp.concatenate([high, low], axis=1)
    pm_ref[...] = tail

    def project(n, _):
        lane = pl.ds(pl.multiple_of(n * size, size), size)
        at = pl.ds(pl.multiple_of(column + n * size, size), size)
        part = jnp.dot(ctx_ref[...], weights[:, at], preferred_element_type=F32)
        out_ref[:, lane] = part.astype(BF16)
        return 0

    lax.fori_loop(0, wide // size, project, 0)
    out_ref[:, wide:] = tail


def attention(lengths, base_q, base_kv, parts, ups, od, angles, keys, values, weights, far):
    rows, kv, positions, dim = keys.shape
    q_cols = base_q.shape[1]
    heads = q_cols // dim
    rank = od.shape[0]
    block = 16 if rows % 16 == 0 else rows
    wide = weights.shape[1] // lax.axis_size("tp")
    vmem = pl.BlockSpec(memory_space=pltpu.VMEM)
    fixed = [base_q, base_kv] + list(ups) + [od] + list(angles) + list(parts)
    scratch = pltpu.VMEM((rows * heads, dim), F32)
    return pl.pallas_call(
        functools.partial(
            attend_kernel, parts=len(parts), group=heads // kv, block=block, far=far
        ),
        in_specs=[pl.BlockSpec(memory_space=pltpu.SMEM)] + [vmem] * (len(fixed) + 3),
        out_specs=[vmem, vmem, vmem],
        scratch_shapes=[
            scratch,
            scratch,
            scratch,
            scratch,
        ],
        out_shape=[
            jax.ShapeDtypeStruct((rows, q_cols), BF16),
            jax.ShapeDtypeStruct((rows, 2 * rank), BF16),
            jax.ShapeDtypeStruct((rows, wide + 2 * rank), BF16),
        ],
        compiler_params=params(8),
        cost_estimate=pl.CostEstimate(
            flops=4 * rows * heads * positions * dim * 16,
            bytes_accessed=4 * keys.size,
            transcendentals=rows * heads * positions,
        ),
        name="attend",
    )(lengths, *fixed, keys, values, weights)


def chunk_kernel(ctx_ref, w_ref, pm_ref, out_ref, *, k):
    wide = out_ref.shape[1] - (pm_ref.shape[1] if k else 0)
    size = 512 if wide % 512 == 0 else wide
    column = chunk_target(k) * wide

    def project(n, _):
        lane = pl.ds(pl.multiple_of(n * size, size), size)
        at = pl.ds(pl.multiple_of(column + n * size, size), size)
        part = jnp.dot(ctx_ref[...], w_ref[:, at], preferred_element_type=F32)
        out_ref[:, lane] = part.astype(out_ref.dtype)
        return 0

    lax.fori_loop(0, wide // size, project, 0)
    if k:
        out_ref[:, wide:] = pm_ref[...]


def chunk(context, weights, middle, k):
    rows, depth = context.shape
    wide = weights.shape[1] // lax.axis_size("tp")
    tail = middle.shape[1] if k else 0
    vmem = pl.BlockSpec(memory_space=pltpu.VMEM)
    return pl.pallas_call(
        functools.partial(chunk_kernel, k=k),
        in_specs=[vmem, vmem, vmem],
        out_specs=vmem,
        out_shape=jax.ShapeDtypeStruct((rows, wide + tail), BF16 if k else F32),
        compiler_params=params(4),
        cost_estimate=pl.CostEstimate(
            flops=2 * rows * depth * wide, bytes_accessed=2 * depth * wide, transcendentals=0
        ),
    )(context, weights, middle)


def relay_kernel(a_ref, b_ref, out_ref, *, tail):
    wide = a_ref.shape[1] - tail
    out_ref[:, :wide] = (a_ref[:, :wide].astype(F32) + b_ref[:, :wide].astype(F32)).astype(BF16)
    half = tail // 2
    ends = a_ref[:, wide:].astype(F32) + b_ref[:, wide:].astype(F32)
    total = ends[:, :half] + ends[:, half:]
    high = total.astype(BF16)
    low = (total - high.astype(F32)).astype(BF16)
    out_ref[:, wide:] = jnp.concatenate([high, low], axis=1)


def add_pieces(a, b, tail):
    vmem = pl.BlockSpec(memory_space=pltpu.VMEM)
    return pl.pallas_call(
        functools.partial(relay_kernel, tail=tail),
        in_specs=[vmem, vmem],
        out_specs=vmem,
        out_shape=jax.ShapeDtypeStruct(a.shape, BF16),
        compiler_params=params(4),
        name="relay",
    )(a, b)


def final_kernel(own_ref, pm_ref, up_ref, *refs):
    others, out_ref = refs[:-1], refs[-1]
    wide = own_ref.shape[1]
    rank = up_ref.shape[0]
    total = own_ref[...]
    middle = pm_ref[:, :rank].astype(F32) + pm_ref[:, rank:].astype(F32)
    for other in others:
        total += other[:, :wide].astype(F32)
        tail = other[:, wide:].astype(F32)
        middle += tail[:, :rank] + tail[:, rank:]
    total += adapter_scale * jnp.dot(
        middle.astype(BF16), up_ref[...], preferred_element_type=F32
    )
    out_ref[...] = total.astype(BF16)


def finish(own, middle, out_up, others):
    args = [own, middle, out_up] + others
    return pl.pallas_call(
        final_kernel,
        grid=(1,),
        in_specs=[whole(a.shape) for a in args],
        out_specs=whole(own.shape),
        out_shape=jax.ShapeDtypeStruct(own.shape, BF16),
        compiler_params=params(8),
        name="final",
    )(*args)


def local(
    hidden,
    norm_gain,
    query_weight_matrix,
    key_value_weight,
    output_weight_matrix,
    input_down_factors,
    query_up_factor,
    key_value_up_factors,
    output_down_factor,
    output_up_factor,
    cache_keys,
    cache_values,
    lengths,
):
    rep = lax.axis_size("rep")
    tp = lax.axis_size("tp")

    head_dim = cache_keys.shape[3]
    count, deep, rank = input_down_factors.shape
    input_down_factors, opened = lax.optimization_barrier((input_down_factors, opening()))
    cosine, sine = tables(lengths, opened, head_dim)
    down = input_down_factors.transpose(0, 2, 1).reshape(count * rank, deep)
    down_blocks = gather_rep(down)
    up_pack, widths = pack(
        query_up_factor, output_down_factor, output_up_factor, key_value_up_factors
    )
    moved = lax.ppermute(
        up_pack, ("rep", "tp"), [(b, (b % rep) * tp + b // rep) for b in range(rep * tp)]
    )
    normed, base_q, base_kv = base_projections(
        hidden, norm_gain, query_weight_matrix, key_value_weight
    )
    moved, base_q = lax.optimization_barrier((moved, base_q))
    up_blocks = gather_rep(moved)
    part = partial_inner(normed, down_blocks)
    parts = [part]
    for k in range(1, tp):
        parts.append(hop(part, "tp", k))
    q_up, od, out_up, k_up, v_up = assemble(up_blocks, widths)
    far = tp - 1
    first = LINE[0] if tp == 4 else far
    context, middle, piece = attention(
        lengths, base_q, base_kv, parts, (q_up, k_up, v_up), od, (cosine, sine),
        cache_keys, cache_values, output_weight_matrix, first,
    )

    def made(target):
        return chunk(context, output_weight_matrix, middle, target)

    def sent(x, pairs):
        return lax.ppermute(x, "tp", pairs)

    if tp == 4:
        across = sent(piece, [(1, 2), (2, 1)])
        relayed = sent(piece, [(0, 1), (3, 2)])
        piece = made(LINE[1])
        second = sent(piece, [(0, 2), (1, 0), (2, 3), (3, 1)])
        piece = made(LINE[2])
        piece = add_pieces(piece, relayed, middle.shape[1])
        others = [across, second, sent(piece, [(0, 1), (1, 3), (2, 0), (3, 2)])]
    else:
        others = [hop(piece, "tp", far)]
        for k in range(far - 1, 0, -1):
            others.append(hop(made(k), "tp", k))
    own = made(0)
    return finish(own, middle, out_up, others)


def solution(mesh):
    return jax.shard_map(
        local,
        mesh=mesh,
        in_specs=(
            P("rep", None),
            P(),
            P(None, "tp"),
            P(None, None, "tp"),
            P("tp", None),
            P(None, ("rep", "tp"), None),
            P(None, ("rep", "tp")),
            P(None, None, ("rep", "tp")),
            P(("rep", "tp"), None),
            P(None, ("rep", "tp")),
            P("rep", "tp", None, None),
            P("rep", "tp", None, None),
            P("rep"),
        ),
        out_specs=P("rep", "tp"),
        check_vma=False,
    )
```

```python
import functools
import math

import jax
import jax.numpy as jnp
from jax import lax
from jax.experimental import pallas as pl
from jax.experimental.pallas import tpu as pltpu
from jax.sharding import PartitionSpec as P


epsilon = 1e-06
rope_base = 1000000.0
adapter_scale = 0.5
F32 = jnp.float32
BF16 = jnp.bfloat16


INNER = 6 * 10**9
LINE = ((3, 2, 1, 0), (2, 0, 3, 1), (1, 3, 0, 2))
LONG = pl.CostEstimate(flops=1 << 34, bytes_accessed=1 << 20, transcendentals=0)


def params(mib=24):
    return pltpu.CompilerParams(vmem_limit_bytes=mib * 1024 * 1024)


def whole(shape):
    return pl.BlockSpec(shape, lambda *_: (0,) * len(shape))


def power_of_two(n):
    return n & (n - 1) == 0


def exchange(n):
    if power_of_two(n):
        return lambda i, k: i ^ k
    return lambda i, k: (i + k) % n


def hop(x, axis, k):
    n = lax.axis_size(axis)
    to = exchange(n)
    return lax.ppermute(x, axis, [(i, to(i, k)) for i in range(n)])


def came_from(index, n, k):
    if power_of_two(n):
        return index ^ k
    return (index - k) % n


def chunk_target(target):
    t = lax.axis_index("tp")
    if isinstance(target, tuple):
        found = target[0]
        for place in range(1, len(target)):
            found = jnp.where(t == place, target[place], found)
        return found
    return exchange(lax.axis_size("tp"))(t, target)


def gather_rep(block):
    n = lax.axis_size("rep")

    def sent(x, k):
        return hop(x, "rep", k)

    if not power_of_two(n) or n == 1:
        return [block] + [sent(block, k) for k in range(1, n)]
    near = [block] + [sent(block, k) for k in range(2, n, 2)]
    swapped = []
    for b in near:
        swapped.append(hop(b, "rep", 1))
    return near + swapped


def rep_order():
    n = lax.axis_size("rep")
    r = lax.axis_index("rep")
    if not power_of_two(n) or n == 1:
        return [came_from(r, n, k) for k in range(n)]
    return [r ^ k for k in range(0, n, 2)] + [r ^ k ^ 1 for k in range(0, n, 2)]


def pack_kernel(q_ref, od_ref, ou_ref, kv_ref, out_ref):
    both = jnp.concatenate([kv_ref[0], kv_ref[1]], axis=0).astype(F32).T.astype(BF16)
    lane = 0
    for piece in (q_ref[...], od_ref[...], ou_ref[...], both):
        out_ref[:, lane : lane + piece.shape[1]] = piece
        lane += piece.shape[1]


def pack(q_up, od, ou, kv_up):
    widths = (q_up.shape[1], od.shape[0], ou.shape[1], kv_up.shape[2], kv_up.shape[2])
    if any(w % 128 for w in widths[:3]):
        return jnp.concatenate([q_up, od.T, ou, kv_up[0], kv_up[1]], axis=1), widths
    vmem = pl.BlockSpec(memory_space=pltpu.VMEM)
    packed = pl.pallas_call(
        pack_kernel,
        in_specs=[vmem] * 4,
        out_specs=vmem,
        out_shape=jax.ShapeDtypeStruct((q_up.shape[0], sum(widths)), BF16),
        compiler_params=params(4),
        name="pack",
    )(q_up, od.T, ou, kv_up.transpose(0, 2, 1))
    return packed, widths


def opening_kernel(out_ref):
    out_ref[...] = jnp.zeros_like(out_ref)


def opening():
    return pl.pallas_call(
        opening_kernel,
        out_specs=pl.BlockSpec(memory_space=pltpu.VMEM),
        out_shape=jax.ShapeDtypeStruct((8, 128), F32),
        compiler_params=params(1),
        cost_estimate=LONG,
        name="opening",
    )()


def tables_kernel(lengths_ref, _, cos_ref, sin_ref, angle):
    rows = cos_ref.shape[0]
    dim = cos_ref.shape[1]
    spot = lax.broadcasted_iota(jnp.int32, (1, dim), 1) % (dim // 2)
    freq = jnp.ones((1, dim), F32)
    for bit in range((dim // 2 - 1).bit_length()):
        power = rope_base ** (-(2.0 ** (bit + 1)) / dim)
        freq *= jnp.where((spot >> bit) % 2 == 1, power, 1.0)
    for s in range(rows):
        angle[s : s + 1, :] = freq * lengths_ref[s].astype(F32)
    low = lax.broadcasted_iota(jnp.int32, (rows, dim), 1) < dim // 2
    wave = jnp.sin(angle[...] + jnp.where(low, 0.0, math.pi / 2))
    other = pltpu.roll(wave, dim // 2, 1)
    cos_ref[...] = jnp.where(low, other, wave)
    sin_ref[...] = jnp.where(low, -wave, other)


def tables(lengths, opened, dim):
    rows = lengths.shape[0]
    vmem = pl.BlockSpec(memory_space=pltpu.VMEM)
    return pl.pallas_call(
        tables_kernel,
        in_specs=[pl.BlockSpec(memory_space=pltpu.SMEM), vmem],
        out_specs=[vmem] * 2,
        out_shape=[jax.ShapeDtypeStruct((rows, dim), F32)] * 2,
        scratch_shapes=[pltpu.VMEM((rows, dim), F32)],
        compiler_params=params(4),
        name="tables",
    )(lengths, opened)


def base_kernel(gain_ref, hidden, q_held, kv_held, x_ref, q_out, kv_out):
    rows, wide = hidden.shape
    depth = wide

    q_out[...] = jnp.zeros_like(q_out)
    kv_out[...] = jnp.zeros_like(kv_out)

    part = gain_ref.shape[1]
    square = jnp.zeros((rows, part), F32)
    for j in range(wide // part):
        states = hidden[:, j * part : (j + 1) * part].astype(F32)
        square += states * states
    factor = lax.rsqrt(jnp.sum(square, axis=-1, keepdims=True) / wide + epsilon)
    for j in range(wide // part):
        lane = slice(j * part, (j + 1) * part)
        scaled = hidden[:, lane].astype(F32) * factor * gain_ref[j : j + 1, :].astype(F32)
        x_ref[:, lane] = scaled.astype(BF16)

    def step(i, _):
        rows_at = pl.ds(pl.multiple_of(i * depth, depth), depth)
        x = x_ref[:, rows_at]
        q_out[...] += jnp.dot(x, q_held[rows_at, :], preferred_element_type=F32)
        for j in range(kv_held.shape[0]):
            kv_out[j] += jnp.dot(x, kv_held[j, rows_at, :], preferred_element_type=F32)
        return 0

    lax.fori_loop(0, wide // depth, step, 0)


def base_projections(hidden, gain, q_weights, kv_weights):
    rows, wide = hidden.shape
    q_cols, kv_cols = q_weights.shape[1], kv_weights.shape[2]
    pair = kv_weights.shape[0]
    vmem = pl.BlockSpec(memory_space=pltpu.VMEM)
    return pl.pallas_call(
        base_kernel,
        in_specs=[vmem] * 4,
        out_specs=[vmem] * 3,
        out_shape=[
            jax.ShapeDtypeStruct((rows, wide), BF16),
            jax.ShapeDtypeStruct((rows, q_cols), F32),
            jax.ShapeDtypeStruct((pair, rows, kv_cols), F32),
        ],
        compiler_params=params(6),
        cost_estimate=pl.CostEstimate(
            flops=16 * rows * (q_weights.size + kv_weights.size),
            bytes_accessed=2 * (q_weights.size + kv_weights.size),
            transcendentals=0,
        ),
        name="base",
    )(gain.reshape(wide // 128, 128), hidden, q_weights, kv_weights)


def inner_kernel(x_ref, *refs):
    blocks, out_ref = refs[:-1], refs[-1]
    order = rep_order()
    tp, t = lax.axis_size("tp"), lax.axis_index("tp")
    ranks, deep = blocks[0].shape
    total = jnp.zeros((x_ref.shape[0], ranks), F32)
    for j, block in enumerate(blocks):
        at = pl.multiple_of((order[j] * tp + t) * deep, deep)
        total += lax.dot_general(
            x_ref[:, pl.ds(at, deep)],
            block[...],
            (((1,), (1,)), ((), ())),
            preferred_element_type=F32,
        )
    rest = jnp.zeros((x_ref.shape[0], out_ref.shape[1] - ranks), F32)
    out_ref[...] = jnp.concatenate([total, rest], axis=1).astype(BF16)


def partial_inner(normed, blocks):
    ranks, deep = blocks[0].shape
    rows = normed.shape[0]
    padded = -(-ranks // 128) * 128
    vmem = pl.BlockSpec(memory_space=pltpu.VMEM)
    if deep % 128 == 0:
        return pl.pallas_call(
            inner_kernel,
            in_specs=[vmem] * (1 + len(blocks)),
            out_specs=vmem,
            out_shape=jax.ShapeDtypeStruct((rows, padded), BF16),
            compiler_params=params(4),
            cost_estimate=pl.CostEstimate(flops=INNER, bytes_accessed=1 << 20, transcendentals=0),
            name="inner",
        )(normed, *blocks)
    total = jnp.zeros((rows, ranks), F32)
    tp, t = lax.axis_size("tp"), lax.axis_index("tp")
    for place, block in zip(rep_order(), blocks):
        place = place * tp + t
        own = lax.dynamic_slice_in_dim(normed, place * deep, deep, 1)
        total += jnp.dot(own, block.T, preferred_element_type=F32)
    return jnp.pad(total, ((0, 0), (0, padded - ranks))).astype(BF16)


def assemble_kernel(*refs, widths, count):
    blocks, outs = refs[:count], refs[count:]
    order = rep_order()
    offset = 0
    for width, out_ref in zip(widths, outs):
        total = out_ref.shape[1]
        if width % 128 == 0:
            for j, block in enumerate(blocks):
                at = pl.multiple_of(order[j] * width, 128)
                out_ref[:, pl.ds(at, width)] = block[:, offset : offset + width]
        else:
            placed = jnp.zeros((out_ref.shape[0], total), F32)
            source = lax.broadcasted_iota(jnp.int32, (width, total), 0)
            target = lax.broadcasted_iota(jnp.int32, (width, total), 1)
            for j, block in enumerate(blocks):
                chosen = (target == source + order[j] * width).astype(BF16)
                placed += jnp.dot(
                    block[:, offset : offset + width], chosen, preferred_element_type=F32
                )
            out_ref[...] = placed.astype(BF16)
        offset += width


def assemble(blocks, widths):
    rank = blocks[0].shape[0]
    count = len(blocks)
    vmem = pl.BlockSpec(memory_space=pltpu.VMEM)
    return pl.pallas_call(
        functools.partial(assemble_kernel, widths=widths, count=count),
        in_specs=[vmem] * count,
        out_specs=[vmem] * len(widths),
        out_shape=[jax.ShapeDtypeStruct((rank, w * count), BF16) for w in widths],
        compiler_params=params(4),
        name="assemble",
    )(*blocks)


def attend_kernel(
    lengths_ref, q_ref, kv_ref, q_up, k_up, v_up, od_ref, cos_ref, sin_ref, *refs,
    parts, group, block, far,
):
    parts_refs = refs[:parts]
    keys, values, weights, ctx_ref, pm_ref, out_ref = refs[parts : parts + 6]
    qs, nk, nv, cs = refs[parts + 6 :]
    rows, dim = cos_ref.shape
    heads = q_ref.shape[1] // dim
    kv = heads // group
    rank = q_up.shape[0]
    scale = 1.0 / math.sqrt(dim)
    count = rows // block
    wide = out_ref.shape[1] - pm_ref.shape[1]
    size = wide
    column = chunk_target(far) * wide

    total = parts_refs[0][...].astype(F32)
    for other in parts_refs[1:]:
        total += other[...].astype(F32)
    inner = total.astype(BF16)
    cosine, sine = cos_ref[...], sin_ref[...]

    def turned(x):
        return x * cosine + pltpu.roll(x, dim // 2, 1) * sine

    def delta(j, up):
        return adapter_scale * jnp.dot(
            inner[:, j * rank : (j + 1) * rank], up[...], preferred_element_type=F32
        )

    key_delta, value_delta, query_delta = delta(1, k_up), delta(2, v_up), delta(0, q_up)
    for g in range(kv):
        lane = slice(g * dim, (g + 1) * dim)
        key = turned(kv_ref[0, :, lane] + key_delta[:, lane]).astype(BF16).astype(F32)
        value = (kv_ref[1, :, lane] + value_delta[:, lane]).astype(BF16).astype(F32)
        for h in range(g * group, (g + 1) * group):
            lane = slice(h * dim, (h + 1) * dim)
            strided = pl.ds(h, rows, stride=heads)
            qs[strided, :] = turned(q_ref[:, lane] + query_delta[:, lane])
            nk[strided, :] = key
            nv[strided, :] = value

    row = lax.broadcasted_iota(jnp.int32, (heads, dim), 0)
    positions = keys.shape[2]
    spot = lax.broadcasted_iota(jnp.int32, (heads, positions), 1)

    def select(pieces):
        out = pieces[0]
        for g in range(1, kv):
            out = jnp.where(row >= g * group, pieces[g], out)
        return out

    def score(i):
        span = slice(i * block * heads, (i + 1) * block * heads)
        query = qs[span, :]
        high = query.astype(BF16)
        rest = query - high.astype(F32)
        mid = rest.astype(BF16)
        low = (rest - mid.astype(F32)).astype(BF16)
        found = []
        for b in range(block):
            s = i * block + b
            at = slice(b * heads, (b + 1) * heads)
            q = jnp.concatenate([high[at], mid[at], low[at]], axis=0)
            pieces = []
            for g in range(kv):
                full = lax.dot_general(
                    q, keys[s, g], (((1,), (1,)), ((), ())), preferred_element_type=F32
                )
                pieces.append(full[:heads] + (full[heads : 2 * heads] + full[2 * heads :]))
            found.append(jnp.where(spot < lengths_ref[s], select(pieces) * scale, -1e30))
        own_score = jnp.sum(query * nk[span, :], axis=-1, keepdims=True) * scale
        return jnp.concatenate(found, axis=0), own_score

    def weigh(scores, own_score):
        top = jnp.maximum(jnp.max(scores, axis=-1, keepdims=True), own_score)
        exps = jnp.exp(scores - top)
        own_weight = jnp.exp(own_score - top)
        inverse = 1.0 / (jnp.sum(exps, axis=-1, keepdims=True) + own_weight)
        return (exps * inverse).astype(BF16), (own_weight * inverse).astype(BF16).astype(F32)

    def gather(i, probs, own_prob):
        span = slice(i * block * heads, (i + 1) * block * heads)
        found = []
        for b in range(block):
            s = i * block + b
            p = probs[b * heads : (b + 1) * heads]
            pieces = [
                jnp.dot(p, values[s, g], preferred_element_type=F32) for g in range(kv)
            ]
            found.append(select(pieces))
        cs[span, :] = jnp.concatenate(found, axis=0) + own_prob * nv[span, :]

    scored, weighed = None, None
    for i in range(count + 2):
        if i >= 2:
            gather(i - 2, *weighed)
        if 1 <= i <= count:
            weighed = weigh(*scored)
        if i < count:
            scored = score(i)

    middle = jnp.zeros((rows, rank), F32)
    for h in range(heads):
        lane = slice(h * dim, (h + 1) * dim)
        context = cs[pl.ds(h, rows, stride=heads), :].astype(BF16)
        ctx_ref[:, lane] = context
        middle += lax.dot_general(
            context, od_ref[:, lane], (((1,), (1,)), ((), ())), preferred_element_type=F32
        )
    high = middle.astype(BF16)
    low = (middle - high.astype(F32)).astype(BF16)
    tail = jnp.concatenate([high, low], axis=1)
    pm_ref[...] = tail

    def project(n, _):
        lane = pl.ds(pl.multiple_of(n * size, size), size)
        at = pl.ds(pl.multiple_of(column + n * size, size), size)
        part = jnp.dot(ctx_ref[...], weights[:, at], preferred_element_type=F32)
        out_ref[:, lane] = part.astype(BF16)
        return 0

    lax.fori_loop(0, wide // size, project, 0)
    out_ref[:, wide:] = tail


def attention(lengths, base_q, base_kv, parts, ups, od, angles, keys, values, weights, far):
    rows, kv, positions, dim = keys.shape
    q_cols = base_q.shape[1]
    heads = q_cols // dim
    rank = od.shape[0]
    block = 16 if rows % 16 == 0 else rows
    wide = weights.shape[1] // lax.axis_size("tp")
    vmem = pl.BlockSpec(memory_space=pltpu.VMEM)
    fixed = [base_q, base_kv] + list(ups) + [od] + list(angles) + list(parts)
    scratch = pltpu.VMEM((rows * heads, dim), F32)
    return pl.pallas_call(
        functools.partial(
            attend_kernel, parts=len(parts), group=heads // kv, block=block, far=far
        ),
        in_specs=[pl.BlockSpec(memory_space=pltpu.SMEM)] + [vmem] * (len(fixed) + 3),
        out_specs=[vmem, vmem, vmem],
        scratch_shapes=[
            scratch,
            scratch,
            scratch,
            scratch,
        ],
        out_shape=[
            jax.ShapeDtypeStruct((rows, q_cols), BF16),
            jax.ShapeDtypeStruct((rows, 2 * rank), BF16),
            jax.ShapeDtypeStruct((rows, wide + 2 * rank), BF16),
        ],
        compiler_params=params(8),
        cost_estimate=pl.CostEstimate(
            flops=4 * rows * heads * positions * dim * 16,
            bytes_accessed=4 * keys.size,
            transcendentals=rows * heads * positions,
        ),
        name="attend",
    )(lengths, *fixed, keys, values, weights)


def chunk_kernel(ctx_ref, w_ref, pm_ref, out_ref, *, k):
    wide = out_ref.shape[1] - (pm_ref.shape[1] if k else 0)
    size = wide
    column = chunk_target(k) * wide

    def project(n, _):
        lane = pl.ds(pl.multiple_of(n * size, size), size)
        at = pl.ds(pl.multiple_of(column + n * size, size), size)
        part = jnp.dot(ctx_ref[...], w_ref[:, at], preferred_element_type=F32)
        out_ref[:, lane] = part.astype(out_ref.dtype)
        return 0

    lax.fori_loop(0, wide // size, project, 0)
    if k:
        out_ref[:, wide:] = pm_ref[...]


def chunk(context, weights, middle, k):
    rows, depth = context.shape
    wide = weights.shape[1] // lax.axis_size("tp")
    tail = middle.shape[1] if k else 0
    vmem = pl.BlockSpec(memory_space=pltpu.VMEM)
    return pl.pallas_call(
        functools.partial(chunk_kernel, k=k),
        in_specs=[vmem, vmem, vmem],
        out_specs=vmem,
        out_shape=jax.ShapeDtypeStruct((rows, wide + tail), BF16 if k else F32),
        compiler_params=params(4),
        cost_estimate=pl.CostEstimate(
            flops=2 * rows * depth * wide, bytes_accessed=2 * depth * wide, transcendentals=0
        ),
    )(context, weights, middle)


def relay_kernel(a_ref, b_ref, out_ref, *, tail):
    wide = a_ref.shape[1] - tail
    out_ref[:, :wide] = (a_ref[:, :wide].astype(F32) + b_ref[:, :wide].astype(F32)).astype(BF16)
    half = tail // 2
    ends = a_ref[:, wide:].astype(F32) + b_ref[:, wide:].astype(F32)
    total = ends[:, :half] + ends[:, half:]
    high = total.astype(BF16)
    low = (total - high.astype(F32)).astype(BF16)
    out_ref[:, wide:] = jnp.concatenate([high, low], axis=1)


def add_pieces(a, b, tail):
    vmem = pl.BlockSpec(memory_space=pltpu.VMEM)
    return pl.pallas_call(
        functools.partial(relay_kernel, tail=tail),
        in_specs=[vmem, vmem],
        out_specs=vmem,
        out_shape=jax.ShapeDtypeStruct(a.shape, BF16),
        compiler_params=params(4),
        name="relay",
    )(a, b)


def final_kernel(own_ref, pm_ref, up_ref, *refs):
    others, out_ref = refs[:-1], refs[-1]
    wide = own_ref.shape[1]
    rank = up_ref.shape[0]
    total = own_ref[...]
    middle = pm_ref[:, :rank].astype(F32) + pm_ref[:, rank:].astype(F32)
    for other in others:
        total += other[:, :wide].astype(F32)
        tail = other[:, wide:].astype(F32)
        middle += tail[:, :rank] + tail[:, rank:]
    total += adapter_scale * jnp.dot(
        middle.astype(BF16), up_ref[...], preferred_element_type=F32
    )
    out_ref[...] = total.astype(BF16)


def finish(own, middle, out_up, others):
    args = [own, middle, out_up] + others
    return pl.pallas_call(
        final_kernel,
        grid=(1,),
        in_specs=[whole(a.shape) for a in args],
        out_specs=whole(own.shape),
        out_shape=jax.ShapeDtypeStruct(own.shape, BF16),
        compiler_params=params(8),
        name="final",
    )(*args)


def local(
    hidden,
    norm_gain,
    query_weight_matrix,
    key_value_weight,
    output_weight_matrix,
    input_down_factors,
    query_up_factor,
    key_value_up_factors,
    output_down_factor,
    output_up_factor,
    cache_keys,
    cache_values,
    lengths,
):
    rep = lax.axis_size("rep")
    tp = lax.axis_size("tp")

    head_dim = cache_keys.shape[3]
    count, deep, rank = input_down_factors.shape
    input_down_factors, opened = lax.optimization_barrier((input_down_factors, opening()))
    cosine, sine = tables(lengths, opened, head_dim)
    down = input_down_factors.transpose(0, 2, 1).reshape(count * rank, deep)
    down_blocks = gather_rep(down)
    up_pack, widths = pack(
        query_up_factor, output_down_factor, output_up_factor, key_value_up_factors
    )
    moved = lax.ppermute(
        up_pack, ("rep", "tp"), [(b, (b % rep) * tp + b // rep) for b in range(rep * tp)]
    )
    normed, base_q, base_kv = base_projections(
        hidden, norm_gain, query_weight_matrix, key_value_weight
    )
    moved, base_q = lax.optimization_barrier((moved, base_q))
    up_blocks = gather_rep(moved)
    part = partial_inner(normed, down_blocks)
    parts = [part]
    for k in range(1, tp):
        parts.append(hop(part, "tp", k))
    q_up, od, out_up, k_up, v_up = assemble(up_blocks, widths)
    far = tp - 1
    first = LINE[0] if tp == 4 else far
    context, middle, piece = attention(
        lengths, base_q, base_kv, parts, (q_up, k_up, v_up), od, (cosine, sine),
        cache_keys, cache_values, output_weight_matrix, first,
    )

    def made(target):
        return chunk(context, output_weight_matrix, middle, target)

    def sent(x, pairs):
        return lax.ppermute(x, "tp", pairs)

    if tp == 4:
        across = sent(piece, [(1, 2), (2, 1)])
        relayed = sent(piece, [(0, 1), (3, 2)])
        piece = made(LINE[1])
        second = sent(piece, [(0, 2), (1, 0), (2, 3), (3, 1)])
        piece = made(LINE[2])
        piece = add_pieces(piece, relayed, middle.shape[1])
        others = [across, second, sent(piece, [(0, 1), (1, 3), (2, 0), (3, 2)])]
    else:
        others = [hop(piece, "tp", far)]
        for k in range(far - 1, 0, -1):
            others.append(hop(made(k), "tp", k))
    own = made(0)
    return finish(own, middle, out_up, others)


def solution(mesh):
    return jax.shard_map(
        local,
        mesh=mesh,
        in_specs=(
            P("rep", None),
            P(),
            P(None, "tp"),
            P(None, None, "tp"),
            P("tp", None),
            P(None, ("rep", "tp"), None),
            P(None, ("rep", "tp")),
            P(None, None, ("rep", "tp")),
            P(("rep", "tp"), None),
            P(None, ("rep", "tp")),
            P("rep", "tp", None, None),
            P("rep", "tp", None, None),
            P("rep"),
        ),
        out_specs=P("rep", "tp"),
        check_vma=False,
    )
```
